32 devices in a mesh: tx: 4 (over x, core), ty: 4 (over z), src: 2 (over y).
Axes of the slice: x: 2, y: 2, z: 4, core: 2. Of those that a mesh axis runs over, the one named last changes fastest.
Arguments:
- spectrum: bfloat16 [2, 512, 512], P(None, ('tx', 'ty'), 'src'), may hold values from -0.0234375 to 0.0234375
- pupil_mask: int32 [256, 256], replicated, may hold values 0 or 1
- source_shifts: int32 [64, 2], P('src'), may hold values from 0 to 256
- source_weights: int32 [64], P('src'), may hold values from 0 to 8, as said below
Outputs:
- acid_level: float32 [2048, 1024], P(('tx', 'src'), 'ty')
The draws below stay inside these ranges and needn't reach their ends.
Inputs may be any that keep to these rules, and one draw needn't show every extreme that they name: `source_weights`: the 32 consecutive sources of each group (one index of src) hold at least 4 points with weight above 0; some group has all 32 points on.
All inputs are finite; a program needn't handle non-finite values.
Results may differ from the reference program's by a relative error of at most 0.0017.
Values may be sent and summed in bfloat16 or wider, within the bound.
A program may use at most 64 MiB of HBM per device.

```python
import jax
import jax.numpy as jnp
from jax import lax

K = 256
MW = 512
FRAME = 2048
SRC_DEV = 32
SOURCES = 64
NX = 2048
NY = 1024


def slot_order(subkey):
    return jax.random.permutation(subkey, SRC_DEV)


def draw_source_weights(key, part):
    group_count = SOURCES // SRC_DEV
    subkeys = jax.random.split(jax.random.fold_in(key, 11), 4)
    counts = jax.random.randint(subkeys[0], (group_count,), SRC_DEV // 8, SRC_DEV // 2 + 1)
    full_group = jax.random.randint(subkeys[1], (), 0, group_count)
    counts = jnp.where(jnp.arange(group_count) == full_group, SRC_DEV, counts)
    slot_rank = jax.vmap(slot_order)(jax.random.split(subkeys[2], group_count))
    levels = jax.random.randint(subkeys[3], (group_count, SRC_DEV), 1, 9)
    levels = levels.at[full_group, 0].set(8)
    chosen = jnp.where(slot_rank < counts[:, None], levels, 0)
    return chosen.reshape(SOURCES).astype(jnp.int32)


def touch_ends(values, key, low, top_value):
    longest = values.shape.index(max(values.shape))
    spots = []
    for shift in (0, 1):
        where = [jax.random.randint(jax.random.fold_in(key, axis), (), 0, length) for axis, length in enumerate(values.shape)]
        where[longest] = (where[longest] + shift) % values.shape[longest]
        spots.append(tuple(where))
    return values.at[spots[0]].set(low).at[spots[1]].set(top_value)


def block_scale(key, dims, shards, least, high):
    factor_of = 1.0
    for dim, parts in shards:
        steps = jax.random.uniform(jax.random.fold_in(jax.random.fold_in(key, 6), dim), (parts,), jnp.float32, least / len(shards), high / len(shards))
        factor_of = factor_of * jnp.repeat(jnp.exp(steps), dims[dim] // parts).reshape((-1,) + (1,) * (len(dims) - 1 - dim))
    return factor_of


def centred(stream_key, shape, spread, most, cuts=(), kind=jnp.bfloat16):
    level = block_scale(stream_key, shape, cuts, -0.22, 0.18) if cuts else 1.0
    entries = jax.random.normal(stream_key, shape, jnp.float32) * spread * level
    return jnp.minimum(jnp.maximum(entries, -most), most).astype(kind)


def setup_inputs(seed: int = 0) -> dict:
    splits = jax.random.split(jax.random.key(seed), 5)
    return {
        "spectrum": centred(splits[0], (2, MW, MW), (K * K) ** -0.5, 0.0234375, ((1, 16), (2, 2))),
        "pupil_mask": touch_ends((jax.random.randint(splits[1], (K, K), 0, 4) < 3).astype(jnp.int32), jax.random.fold_in(splits[1], 1), 0, 1),
        "source_shifts": touch_ends(jax.random.randint(splits[2], (SOURCES, 2), 0, MW - K + 1), jax.random.fold_in(splits[2], 1), 0, MW - K).astype(jnp.int32),
        "source_weights": draw_source_weights(jax.random.fold_in(splits[4], 71), 0),
    }


diffusion_rate = 0.2


def phase_table(positions, frequency_count, frame_points):
    frequency = jnp.arange(frequency_count, dtype=jnp.int32) - frequency_count // 2
    phase_turns = (positions[:, None] * frequency[None, :]) % frame_points
    phase_angle = phase_turns.astype(jnp.float32) * (2.0 * jnp.pi / frame_points)
    return jnp.cos(phase_angle), jnp.sin(phase_angle)


def rotation_table(cosine, sine):
    upper = jnp.concatenate([cosine, -sine], axis=1)
    lower = jnp.concatenate([sine, cosine], axis=1)
    return jnp.concatenate([upper, lower], axis=0).astype(jnp.bfloat16)


def diffuse(level, padded):
    beside = padded[2:, 1:-1] + padded[:-2, 1:-1] + padded[1:-1, 2:] + padded[1:-1, :-2]
    return level + diffusion_rate * (beside - 4.0 * level)


def reference(spectrum, pupil_mask, source_shifts, source_weights):
    passband = pupil_mask.shape[0]
    pupil_bf = pupil_mask.astype(jnp.bfloat16)
    row_cos, row_sin = phase_table(jnp.arange(NX, dtype=jnp.int32), passband, FRAME)
    row_table = rotation_table(row_cos, row_sin).astype(jnp.float32)
    col_cos, col_sin = phase_table(jnp.arange(NY, dtype=jnp.int32), passband, FRAME)
    col_table = jnp.concatenate([col_cos.T, col_sin.T], axis=1).astype(jnp.bfloat16).astype(jnp.float32)

    def one_source(running, item):
        shift_pair, weight_value = item
        window_cut = lax.dynamic_slice(spectrum, (jnp.int32(0), shift_pair[0].astype(jnp.int32), shift_pair[1].astype(jnp.int32)), (2, passband, passband)) * pupil_bf
        product = jnp.dot(window_cut.reshape(2 * passband, passband).astype(jnp.float32), col_table)
        real_part = product[:passband, :NY] - product[passband:, NY:]
        imag_part = product[:passband, NY:] + product[passband:, :NY]
        inner_block = jnp.concatenate([real_part, imag_part], axis=0).astype(jnp.bfloat16)
        field_pair = jnp.dot(row_table, inner_block.astype(jnp.float32))
        square = field_pair[:NX] ** 2 + field_pair[NX:] ** 2
        return running + weight_value.astype(jnp.float32) * square, None

    intensity_sum, _ = lax.scan(one_source, jnp.zeros((NX, NY), jnp.float32), (source_shifts, source_weights))
    intensity = intensity_sum / (2.0 * SOURCES)
    acid_level = 1.0 - jnp.exp(-intensity)
    for repeat in range(2):
        padded = jnp.pad(acid_level, 1)
        acid_level = diffuse(acid_level, padded)
    return acid_level
```

```python
import functools

import jax
import jax.numpy as jnp
from jax import lax
from jax.experimental import pallas as pl
from jax.experimental.pallas import tpu as pltpu
from jax.sharding import PartitionSpec as P

FRAME = 2048
BY = 256
LANES = 128
GROUP = 2
MESH = pl.DeviceIdType.MESH

diffusion_rate = 0.2


def half_angle(odd, positions):
    turns = (odd * positions) % (2 * FRAME)
    return turns.astype(jnp.float32) * (jnp.pi / FRAME)


def tables(row_count, col_count, half):
    row_block = lax.axis_index("tx") * lax.axis_size("src") + lax.axis_index("src")
    odd = 2 * jnp.arange(half, dtype=jnp.int32) + 1
    rows = row_block * row_count + jnp.arange(row_count, dtype=jnp.int32)
    cols = lax.axis_index("ty") * col_count + jnp.arange(col_count, dtype=jnp.int32)
    row_angle = half_angle(odd[None, :], rows[:, None])
    col_angle = half_angle(odd[:, None], cols[None, :])
    row_table = jnp.concatenate([jnp.cos(row_angle), jnp.sin(row_angle)], axis=1)
    col_table = jnp.concatenate([jnp.cos(col_angle), jnp.sin(col_angle)], axis=0)
    return row_table.astype(jnp.bfloat16), col_table.astype(jnp.bfloat16)


def dot(a, b):
    return jnp.dot(a, b, preferred_element_type=jnp.float32)


def reversal(size):
    rows = lax.broadcasted_iota(jnp.int32, (size, size), 0)
    cols = lax.broadcasted_iota(jnp.int32, (size, size), 1)
    return jnp.where(rows + cols == size - 1, 1.0, 0.0).astype(jnp.bfloat16)


def image_kernel(
    shifts, weights, spec_ref, pupil_ref, row_ref, col_ref, out_ref, flips, masks, acc, live, live_weight
):
    source_count = weights.shape[0]
    mask_width = spec_ref.shape[1]
    half = pupil_ref.shape[0] // 2
    tiles = mask_width // LANES
    block = 256

    turn = reversal(block)
    for plane in range(2):
        for i in range(mask_width // block):
            for j in range(mask_width // block):
                ri, rj = mask_width // block - 1 - i, mask_width // block - 1 - j
                cell = spec_ref[plane, block * i : block * (i + 1), block * j : block * (j + 1)]
                col_flip = dot(cell, turn)
                row_flip = dot(turn, cell)
                both = dot(turn, col_flip.astype(jnp.bfloat16))
                for version, value, vi, vj in (
                    (0, cell.astype(jnp.float32), i, j),
                    (1, row_flip, ri, j),
                    (2, col_flip, i, rj),
                    (3, both, ri, rj),
                ):
                    for t in range(block // LANES):
                        slot = (version * 2 + plane) * tiles + vj * (block // LANES) + t
                        flips[slot, block * vi : block * (vi + 1), :] = value[:, LANES * t : LANES * (t + 1)]
    small = reversal(half)
    pupil = pupil_ref[...].astype(jnp.float32).astype(jnp.bfloat16)
    masks[0] = pupil[half:, half:].astype(jnp.float32)
    masks[1] = dot(small, pupil[:half, half:])
    masks[2] = dot(pupil[half:, :half], small)
    masks[3] = dot(small, dot(pupil[:half, :half], small).astype(jnp.bfloat16))

    def clear(i, carry):
        live[i] = 0
        live_weight[i] = 0
        return carry

    lax.fori_loop(0, source_count + GROUP, clear, 0)

    def pick(i, count):
        weight = weights[i]
        live[count] = i
        live_weight[count] = jnp.maximum(weight, 0)
        return count + (weight > 0).astype(jnp.int32)

    count = lax.fori_loop(0, source_count, pick, jnp.int32(0))
    live_weight[count] = 0

    acc[...] = jnp.zeros_like(acc)
    lane = lax.broadcasted_iota(jnp.int32, (half, LANES), 1)

    def fold(a, b):
        row_offsets = (a + half, mask_width - half - a)
        col_offsets = (b + half, mask_width - half - b)
        parts = []
        for plane in range(2):
            quads = []
            for col_side in range(2):
                off = col_offsets[col_side]
                tile, rest = off // LANES, off % LANES
                after = jnp.minimum(tile + 1, tiles - 1)
                back = (LANES - rest) % LANES
                for row_side in range(2):
                    version = 2 * col_side + row_side
                    base = (version * 2 + plane) * tiles
                    rows = pl.ds(row_offsets[row_side], half)
                    left = flips[base + tile, rows, :]
                    right = flips[base + after, rows, :]
                    merged = jnp.where(lane >= rest, left, right)
                    quads.append(pltpu.roll(merged, back, 1) * masks[version])
            s1, d1 = quads[0] + quads[1], quads[0] - quads[1]
            s2, d2 = quads[2] + quads[3], quads[2] - quads[3]
            parts.append((s1, d1, s2, d2))
        (s1, d1, s2, d2), (t1, e1, t2, e2) = parts
        return (
            jnp.concatenate([s1 + s2, t2 - t1], axis=1),
            jnp.concatenate([-(e1 + e2), d2 - d1], axis=1),
            jnp.concatenate([t1 + t2, s1 - s2], axis=1),
            jnp.concatenate([d1 + d2, e2 - e1], axis=1),
        )

    def turn_body(step, carry):
        total = jnp.zeros(acc.shape, jnp.float32)
        for g in range(GROUP):
            index = step * GROUP + g
            source = live[index]
            weight = live_weight[index].astype(jnp.float32)
            folded = jnp.concatenate(fold(shifts[source, 0], shifts[source, 1]), axis=0).astype(jnp.bfloat16)
            inner = dot(folded, col_ref[...]).astype(jnp.bfloat16)
            real = dot(row_ref[...], inner[: 2 * half])
            imag = dot(row_ref[...], inner[2 * half :])
            total = total + weight * (real * real + imag * imag)
        acc[...] += total
        return carry

    lax.fori_loop(0, (count + GROUP - 1) // GROUP, turn_body, 0)
    out_ref[...] = 1.0 - jnp.exp(-(acc[...] / (2.0 * source_count)))


def image(shifts, weights, spectrum, pupil_mask, row_table, col_table):
    source_count = weights.shape[0]
    mask_width = spectrum.shape[1]
    half = pupil_mask.shape[0] // 2
    tile = (row_table.shape[0], col_table.shape[1])
    smem = pl.BlockSpec(memory_space=pltpu.SMEM)
    vmem = pl.BlockSpec(memory_space=pltpu.VMEM)
    return pl.pallas_call(
        image_kernel,
        out_shape=jax.ShapeDtypeStruct(tile, jnp.float32),
        in_specs=[smem, smem, vmem, vmem, vmem, vmem],
        out_specs=vmem,
        scratch_shapes=[
            pltpu.VMEM((8 * mask_width // LANES, mask_width, LANES), jnp.float32),
            pltpu.VMEM((4, half, half), jnp.float32),
            pltpu.VMEM(tile, jnp.float32),
            pltpu.SMEM((source_count + GROUP,), jnp.int32),
            pltpu.SMEM((source_count + GROUP,), jnp.int32),
        ],
        name="image",
    )(shifts, weights, spectrum, pupil_mask, row_table, col_table)


def diffuse_kernel(sizes, acid_ref, out_ref, strips, corners, edges, beside, send_sem, recv_sem):
    tx_count, ty_count, src_count = sizes
    rows, cols = acid_ref.shape
    row_block = lax.axis_index("tx") * src_count + lax.axis_index("src")
    col_block = lax.axis_index("ty")
    row_blocks = tx_count * src_count

    def device(dr, dc):
        other = lax.rem(row_block + row_blocks + dr, row_blocks)
        return {
            "tx": other // src_count,
            "src": lax.rem(other, src_count),
            "ty": lax.rem(col_block + ty_count + dc, ty_count),
        }

    around = [(dr, dc) for dr in (-1, 0, 1) for dc in (-1, 0, 1) if (dr, dc) != (0, 0)]
    barrier = pltpu.get_barrier_semaphore()
    for dr, dc in around:
        pl.semaphore_signal(barrier, inc=1, device_id=device(dr, dc), device_id_type=MESH)
    strips[0] = acid_ref[:, :LANES].T[:8]
    strips[1] = acid_ref[:, cols - LANES :].T[LANES - 8 :]
    pl.semaphore_wait(barrier, len(around))

    copies = []
    for n, (dr, dc) in enumerate(around):
        if dc == 0:
            src = acid_ref.at[:8] if dr < 0 else acid_ref.at[rows - 8 :]
            dst = edges.at[0 if dr > 0 else 1]
        elif dr == 0:
            src = strips.at[0 if dc < 0 else 1]
            dst = beside.at[0 if dc > 0 else 1]
        else:
            row_part = slice(0, 8) if dr < 0 else slice(rows - 8, rows)
            col_part = slice(0, LANES) if dc < 0 else slice(cols - LANES, cols)
            src = acid_ref.at[row_part, col_part]
            dst = corners.at[(0 if dr > 0 else 2) + (0 if dc > 0 else 1)]
        copy = pltpu.make_async_remote_copy(
            src_ref=src,
            dst_ref=dst,
            send_sem=send_sem.at[n],
            recv_sem=recv_sem.at[n],
            device_id=device(dr, dc),
            device_id_type=MESH,
        )
        copy.start()
        copies.append(copy)
    for copy in copies:
        copy.wait()

    none = jnp.zeros((LANES - 8, rows), jnp.float32)
    left = jnp.concatenate([none, beside[0]], axis=0).T
    right = jnp.concatenate([beside[1], none], axis=0).T
    level = jnp.concatenate(
        [
            jnp.concatenate([corners[0], edges[0], corners[1]], axis=1),
            jnp.concatenate([left, acid_ref[...], right], axis=1),
            jnp.concatenate([corners[2], edges[1], corners[3]], axis=1),
        ],
        axis=0,
    )
    x = row_block * rows - 8 + lax.broadcasted_iota(jnp.int32, level.shape, 0)
    y = col_block * cols - LANES + lax.broadcasted_iota(jnp.int32, level.shape, 1)
    inside = (x >= 0) & (x < row_blocks * rows) & (y >= 0) & (y < ty_count * cols)
    tall, wide = level.shape
    for repeat in range(2):
        level = jnp.where(inside, level, 0.0)
        near = (
            pltpu.roll(level, 1, 0)
            + pltpu.roll(level, tall - 1, 0)
            + pltpu.roll(level, 1, 1)
            + pltpu.roll(level, wide - 1, 1)
        )
        level = level + diffusion_rate * (near - 4.0 * level)
    out_ref[...] = level[8 : 8 + rows, LANES : LANES + cols]


def diffuse(acid, sizes):
    rows, cols = acid.shape
    vmem = pl.BlockSpec(memory_space=pltpu.VMEM)
    return pl.pallas_call(
        functools.partial(diffuse_kernel, sizes),
        out_shape=jax.ShapeDtypeStruct((rows, cols), jnp.float32),
        in_specs=[vmem],
        out_specs=vmem,
        scratch_shapes=[
            pltpu.VMEM((2, 8, rows), jnp.float32),
            pltpu.VMEM((4, 8, LANES), jnp.float32),
            pltpu.VMEM((2, 8, cols), jnp.float32),
            pltpu.VMEM((2, 8, rows), jnp.float32),
            pltpu.SemaphoreType.DMA((8,)),
            pltpu.SemaphoreType.DMA((8,)),
        ],
        compiler_params=pltpu.CompilerParams(collective_id=1, has_side_effects=True),
        name="diffuse",
    )(acid)


def body(sizes, spectrum, pupil_mask, source_shifts, source_weights):
    partial_spec = lax.all_gather(spectrum, "src", axis=2, tiled=True)
    spectrum_all = lax.all_gather(partial_spec, ("tx", "ty"), axis=1, tiled=True)
    shifts = lax.all_gather(source_shifts, "src", axis=0, tiled=True)
    weights = lax.all_gather(source_weights, "src", axis=0, tiled=True)
    tx_count, ty_count, src_count = sizes
    rows = FRAME // (tx_count * src_count)
    row_table, col_table = tables(rows, BY, pupil_mask.shape[0] // 2)
    acid = image(shifts, weights, spectrum_all, pupil_mask, row_table, col_table)
    return diffuse(acid, sizes)


def solution(mesh):
    sizes = (mesh.shape["tx"], mesh.shape["ty"], mesh.shape["src"])
    placed = (P(None, ("tx", "ty"), "src"), P(), P("src", None), P("src"))
    return jax.shard_map(
        functools.partial(body, sizes),
        mesh=mesh,
        in_specs=placed,
        out_specs=P(("tx", "src"), "ty"),
        check_vma=False,
    )
```

```python
import functools

import jax
import jax.numpy as jnp
from jax import lax
from jax.experimental import pallas as pl
from jax.experimental.pallas import tpu as pltpu
from jax.sharding import PartitionSpec as P

FRAME = 2048
BY = 256
LANES = 128
GROUP = 2
MESH = pl.DeviceIdType.MESH

diffusion_rate = 0.2


def half_angle(odd, positions):
    turns = (odd * positions) & (2 * FRAME - 1)
    return turns.astype(jnp.float32) * (jnp.pi / FRAME)


def iota(shape, dim):
    return lax.broadcasted_iota(jnp.int32, shape, dim)


def dot(a, b):
    return jnp.dot(a, b, preferred_element_type=jnp.float32)


def reversal(size):
    rows = lax.broadcasted_iota(jnp.int32, (size, size), 0)
    cols = lax.broadcasted_iota(jnp.int32, (size, size), 1)
    return jnp.where(rows + cols == size - 1, 1.0, 0.0).astype(jnp.bfloat16)


def gather_kernel(
    sizes, spec_ref, shift_ref, weight_ref, pupil_ref, all_ref, shifts_ref, weights_ref, row_ref, col_ref, mask_ref,
    send_sem, recv_sem, side_send, side_recv,
):
    tx_count, ty_count, src_count = sizes
    pair_count = tx_count // 2
    tx, t, s = lax.axis_index("tx"), lax.axis_index("ty"), lax.axis_index("src")
    pair, core = tx // 2, lax.rem(tx, 2)
    other_core = 1 - core
    far_t = [lax.rem(t + d, ty_count) for d in range(1, ty_count)]
    far_s = [lax.rem(s + d, src_count) for d in range(1, src_count)]
    far_pair = [lax.rem(pair + d, pair_count) for d in range(1, pair_count)]

    def along_ty(i):
        return {"tx": tx, "ty": i, "src": s}

    def along_src(i):
        return {"tx": tx, "ty": t, "src": i}

    def along_pair(i):
        return {"tx": 2 * i + core, "ty": t, "src": s}

    across = {"tx": 2 * pair + other_core, "ty": t, "src": s}
    partners = [along_ty(i) for i in far_t] + [along_src(i) for i in far_s]
    partners += [along_pair(i) for i in far_pair] + [across]
    barrier = pltpu.get_barrier_semaphore()
    for partner in partners:
        pl.semaphore_signal(barrier, inc=1, device_id=partner, device_id_type=MESH)
    pl.semaphore_wait(barrier, len(partners))

    started = []

    def send(plane, piece, device):
        i, j, k = piece
        slot = all_ref.at[k, plane, i, j]
        own = i is tx and j is t and k is s
        copy = pltpu.make_async_remote_copy(
            src_ref=spec_ref.at[plane] if own else slot,
            dst_ref=slot,
            send_sem=send_sem.at[len(started)],
            recv_sem=recv_sem.at[plane, k, i, j],
            device_id=device,
            device_id_type=MESH,
        )
        copy.start()
        started.append(copy)

    def arrive(plane, piece):
        i, j, k = piece
        slot = all_ref.at[k, plane, i, j]
        pltpu.make_async_remote_copy(
            src_ref=slot,
            dst_ref=slot,
            send_sem=send_sem.at[0],
            recv_sem=recv_sem.at[plane, k, i, j],
            device_id=across,
            device_id_type=MESH,
        ).wait_recv()

    side = []
    for n, i in enumerate(far_s):
        for m, (src, dst) in enumerate(((shift_ref, shifts_ref), (weight_ref, weights_ref))):
            copy = pltpu.make_async_remote_copy(
                src_ref=src,
                dst_ref=dst.at[s],
                send_sem=side_send.at[m, n],
                recv_sem=side_recv.at[m, s],
                device_id=along_src(i),
                device_id_type=MESH,
            )
            copy.start()
            side.append(copy)

    def spread(plane, piece):
        for i in far_s:
            send(plane, piece, along_src(i))
        for i in far_pair:
            send(plane, piece, along_pair(i))
        send(plane, piece, across)

    own = (tx, t, s)
    for plane in range(2):
        for i in far_t:
            send(plane, own, along_ty(i))
    for plane in range(2):
        spread(plane, own)

    shifts_ref[s] = shift_ref[...]
    weights_ref[s] = weight_ref[...]
    for plane in range(2):
        all_ref[s, plane, tx, t] = spec_ref[plane]
    half = pupil_ref.shape[0] // 2
    rows, cols = row_ref.shape[0], col_ref.shape[1]
    x = (tx * src_count + s) * rows + iota((rows, half), 0)
    row_angle = half_angle(2 * iota((rows, half), 1) + 1, x)
    row_ref[:, :half] = jnp.cos(row_angle).astype(jnp.bfloat16)
    row_ref[:, half:] = jnp.sin(row_angle).astype(jnp.bfloat16)
    y = t * cols + iota((half, cols), 1)
    col_angle = half_angle(2 * iota((half, cols), 0) + 1, y)
    col_ref[:half] = jnp.cos(col_angle).astype(jnp.bfloat16)
    col_ref[half:] = jnp.sin(col_angle).astype(jnp.bfloat16)
    small = reversal(half)
    pupil = pupil_ref[...].astype(jnp.float32).astype(jnp.bfloat16)
    mask_ref[0] = pupil[half:, half:].astype(jnp.float32)
    mask_ref[1] = dot(small, pupil[:half, half:])
    mask_ref[2] = dot(pupil[half:, :half], small)
    mask_ref[3] = dot(small, dot(pupil[:half, :half], small).astype(jnp.bfloat16))

    near_first = [t] + far_t
    for j in far_t:
        for plane in range(2):
            arrive(plane, (tx, j, s))
            spread(plane, (tx, j, s))
    for j in near_first:
        for k in far_s:
            arrive(0, (tx, j, k))
            for i in far_pair:
                send(0, (tx, j, k), along_pair(i))
            send(0, (tx, j, k), across)
        for i in far_pair:
            there = 2 * i + core
            arrive(1, (there, j, s))
            for k in far_s:
                send(1, (there, j, s), along_src(k))
            send(1, (there, j, s), across)
        for k in far_s:
            arrive(1, (tx, j, k))
            send(1, (tx, j, k), across)
        for i in far_pair:
            arrive(0, (2 * i + core, j, s))
            send(0, (2 * i + core, j, s), across)
    for j in near_first:
        for i in far_pair:
            for k in far_s:
                for plane in range(2):
                    arrive(plane, (2 * i + core, j, k))
                    send(plane, (2 * i + core, j, k), across)
    for j in near_first:
        for i in [pair] + far_pair:
            for k in [s] + far_s:
                for plane in range(2):
                    arrive(plane, (2 * i + other_core, j, k))
    for n, i in enumerate(far_s):
        for m, (src, dst) in enumerate(((shift_ref, shifts_ref), (weight_ref, weights_ref))):
            pltpu.make_async_remote_copy(
                src_ref=src,
                dst_ref=dst.at[i],
                send_sem=side_send.at[m, n],
                recv_sem=side_recv.at[m, i],
                device_id=across,
                device_id_type=MESH,
            ).wait_recv()
    for copy in started + side:
        copy.wait_send()


def gather(spectrum, source_shifts, source_weights, pupil_mask, sizes):
    tx_count, ty_count, src_count = sizes
    pair_count = tx_count // 2
    _, block_rows, block_cols = spectrum.shape
    slots = source_weights.shape[0]
    half = pupil_mask.shape[0] // 2
    rows = FRAME // (tx_count * src_count)
    vmem = pl.BlockSpec(memory_space=pltpu.VMEM)
    lines = pair_count * src_count * ty_count
    sends = 2 * (ty_count - 1) + 2 * lines + 2 * ty_count * (src_count - 1 + pair_count - 1)
    sends += 2 * ty_count * (src_count - 1) * (pair_count - 1)
    return pl.pallas_call(
        functools.partial(gather_kernel, sizes),
        out_shape=(
            jax.ShapeDtypeStruct((src_count, 2, tx_count, ty_count, block_rows, block_cols), jnp.bfloat16),
            jax.ShapeDtypeStruct((src_count, slots, 2), jnp.int32),
            jax.ShapeDtypeStruct((src_count, 1, slots), jnp.int32),
            jax.ShapeDtypeStruct((rows, 2 * half), jnp.bfloat16),
            jax.ShapeDtypeStruct((2 * half, BY), jnp.bfloat16),
            jax.ShapeDtypeStruct((4, half, half), jnp.float32),
        ),
        in_specs=[vmem] * 4,
        out_specs=(vmem,) * 6,
        scratch_shapes=[
            pltpu.SemaphoreType.DMA((sends,)),
            pltpu.SemaphoreType.DMA((2, src_count, tx_count, ty_count)),
            pltpu.SemaphoreType.DMA((2, src_count)),
            pltpu.SemaphoreType.DMA((2, src_count)),
        ],
        compiler_params=pltpu.CompilerParams(collective_id=0, has_side_effects=True),
        name="gather",
    )(spectrum, source_shifts, source_weights[None], pupil_mask)


def image_kernel(
    shifts, weights, spec_ref, masks, row_ref, col_ref, out_ref, flips, acc, live_row, live_col, live_weight
):
    src_count, _, slots = weights.shape
    source_count = src_count * slots
    mask_width = spec_ref.shape[2]
    part = spec_ref.shape[3]
    half = masks.shape[1]
    tiles = mask_width // LANES
    block = 256

    turn = reversal(block)
    for plane in range(2):
        for i in range(mask_width // block):
            for j in range(mask_width // block):
                ri, rj = mask_width // block - 1 - i, mask_width // block - 1 - j
                rows = slice(block * i, block * (i + 1))
                cells = [spec_ref[k, plane, rows] for k in range(block * j // part, -(-block * (j + 1) // part))]
                cell = cells[0] if len(cells) == 1 else jnp.concatenate(cells, axis=1)
                col_flip = dot(cell, turn)
                row_flip = dot(turn, cell)
                both = dot(turn, col_flip.astype(jnp.bfloat16))
                for version, value, vi, vj in (
                    (0, cell.astype(jnp.float32), i, j),
                    (1, row_flip, ri, j),
                    (2, col_flip, i, rj),
                    (3, both, ri, rj),
                ):
                    for t in range(block // LANES):
                        slot = (version * 2 + plane) * tiles + vj * (block // LANES) + t
                        flips[slot, block * vi : block * (vi + 1), :] = value[:, LANES * t : LANES * (t + 1)]

    def pick(i, count):
        group, slot = i // slots, lax.rem(i, slots)
        weight = weights[group, 0, slot]
        live_row[count] = shifts[group, slot, 0]
        live_col[count] = shifts[group, slot, 1]
        live_weight[count] = weight
        return count + (weight > 0).astype(jnp.int32)

    count = lax.fori_loop(0, source_count, pick, jnp.int32(0))
    for g in range(GROUP):
        live_row[count + g] = 0
        live_col[count + g] = 0
        live_weight[count + g] = 0

    acc[...] = jnp.zeros_like(acc)
    lane = lax.broadcasted_iota(jnp.int32, (half, LANES), 1)

    def fold(a, b):
        row_offsets = (a + half, mask_width - half - a)
        col_offsets = (b + half, mask_width - half - b)
        parts = []
        for plane in range(2):
            quads = []
            for col_side in range(2):
                off = col_offsets[col_side]
                tile, rest = off // LANES, off % LANES
                after = jnp.minimum(tile + 1, tiles - 1)
                back = (LANES - rest) % LANES
                for row_side in range(2):
                    version = 2 * col_side + row_side
                    base = (version * 2 + plane) * tiles
                    rows = pl.ds(row_offsets[row_side], half)
                    left = flips[base + tile, rows, :]
                    right = flips[base + after, rows, :]
                    merged = jnp.where(lane >= rest, left, right)
                    quads.append(pltpu.roll(merged, back, 1) * masks[version])
            s1, d1 = quads[0] + quads[1], quads[0] - quads[1]
            s2, d2 = quads[2] + quads[3], quads[2] - quads[3]
            parts.append((s1, d1, s2, d2))
        (s1, d1, s2, d2), (t1, e1, t2, e2) = parts
        return (
            jnp.concatenate([s1 + s2, t2 - t1], axis=1),
            jnp.concatenate([-(e1 + e2), d2 - d1], axis=1),
            jnp.concatenate([t1 + t2, s1 - s2], axis=1),
            jnp.concatenate([d1 + d2, e2 - e1], axis=1),
        )

    def turn_body(step, carry):
        total = jnp.zeros(acc.shape, jnp.float32)
        for g in range(GROUP):
            index = step * GROUP + g
            weight = live_weight[index].astype(jnp.float32)
            folded = jnp.concatenate(fold(live_row[index], live_col[index]), axis=0).astype(jnp.bfloat16)
            inner = dot(folded, col_ref[...]).astype(jnp.bfloat16)
            real = dot(row_ref[...], inner[: 2 * half])
            imag = dot(row_ref[...], inner[2 * half :])
            total = total + weight * (real * real + imag * imag)
        acc[...] += total
        return carry

    lax.fori_loop(0, (count + GROUP - 1) // GROUP, turn_body, 0)
    out_ref[...] = 1.0 - jnp.exp(-(acc[...] / (2.0 * source_count)))


def image(spectrum, shifts, weights, row_table, col_table, masks):
    source_count = weights.shape[0] * weights.shape[2]
    mask_width = spectrum.shape[2]
    tile = (row_table.shape[0], col_table.shape[1])
    smem = pl.BlockSpec(memory_space=pltpu.SMEM)
    vmem = pl.BlockSpec(memory_space=pltpu.VMEM)
    return pl.pallas_call(
        image_kernel,
        out_shape=jax.ShapeDtypeStruct(tile, jnp.float32),
        in_specs=[smem, smem, vmem, vmem, vmem, vmem],
        out_specs=vmem,
        scratch_shapes=[
            pltpu.VMEM((8 * mask_width // LANES, mask_width, LANES), jnp.float32),
            pltpu.VMEM(tile, jnp.float32),
        ]
        + [pltpu.SMEM((source_count + GROUP,), jnp.int32)] * 3,
        name="image",
    )(shifts, weights, spectrum, masks, row_table, col_table)


def diffuse_kernel(sizes, acid_ref, out_ref, strips, corners, edges, beside, send_sem, recv_sem):
    tx_count, ty_count, src_count = sizes
    rows, cols = acid_ref.shape
    row_block = lax.axis_index("tx") * src_count + lax.axis_index("src")
    col_block = lax.axis_index("ty")
    row_blocks = tx_count * src_count

    def device(dr, dc):
        other = lax.rem(row_block + row_blocks + dr, row_blocks)
        return {
            "tx": other // src_count,
            "src": lax.rem(other, src_count),
            "ty": lax.rem(col_block + ty_count + dc, ty_count),
        }

    around = [(dr, dc) for dr in (-1, 0, 1) for dc in (-1, 0, 1) if (dr, dc) != (0, 0)]
    barrier = pltpu.get_barrier_semaphore()
    for dr, dc in around:
        pl.semaphore_signal(barrier, inc=1, device_id=device(dr, dc), device_id_type=MESH)
    strips[0] = acid_ref[:, :LANES].T[:8]
    strips[1] = acid_ref[:, cols - LANES :].T[LANES - 8 :]
    pl.semaphore_wait(barrier, len(around))

    copies = []
    for n, (dr, dc) in enumerate(around):
        if dc == 0:
            src = acid_ref.at[:8] if dr < 0 else acid_ref.at[rows - 8 :]
            dst = edges.at[0 if dr > 0 else 1]
        elif dr == 0:
            src = strips.at[0 if dc < 0 else 1]
            dst = beside.at[0 if dc > 0 else 1]
        else:
            row_part = slice(0, 8) if dr < 0 else slice(rows - 8, rows)
            col_part = slice(0, LANES) if dc < 0 else slice(cols - LANES, cols)
            src = acid_ref.at[row_part, col_part]
            dst = corners.at[(0 if dr > 0 else 2) + (0 if dc > 0 else 1)]
        copy = pltpu.make_async_remote_copy(
            src_ref=src,
            dst_ref=dst,
            send_sem=send_sem.at[n],
            recv_sem=recv_sem.at[n],
            device_id=device(dr, dc),
            device_id_type=MESH,
        )
        copy.start()
        copies.append(copy)
    for copy in copies:
        copy.wait()

    none = jnp.zeros((LANES - 8, rows), jnp.float32)
    left = jnp.concatenate([none, beside[0]], axis=0).T
    right = jnp.concatenate([beside[1], none], axis=0).T
    level = jnp.concatenate(
        [
            jnp.concatenate([corners[0], edges[0], corners[1]], axis=1),
            jnp.concatenate([left, acid_ref[...], right], axis=1),
            jnp.concatenate([corners[2], edges[1], corners[3]], axis=1),
        ],
        axis=0,
    )
    x = row_block * rows - 8 + lax.broadcasted_iota(jnp.int32, level.shape, 0)
    y = col_block * cols - LANES + lax.broadcasted_iota(jnp.int32, level.shape, 1)
    inside = (x >= 0) & (x < row_blocks * rows) & (y >= 0) & (y < ty_count * cols)
    tall, wide = level.shape
    for repeat in range(2):
        level = jnp.where(inside, level, 0.0)
        near = (
            pltpu.roll(level, 1, 0)
            + pltpu.roll(level, tall - 1, 0)
            + pltpu.roll(level, 1, 1)
            + pltpu.roll(level, wide - 1, 1)
        )
        level = level + diffusion_rate * (near - 4.0 * level)
    out_ref[...] = level[8 : 8 + rows, LANES : LANES + cols]


def diffuse(acid, sizes):
    rows, cols = acid.shape
    vmem = pl.BlockSpec(memory_space=pltpu.VMEM)
    return pl.pallas_call(
        functools.partial(diffuse_kernel, sizes),
        out_shape=jax.ShapeDtypeStruct((rows, cols), jnp.float32),
        in_specs=[vmem],
        out_specs=vmem,
        scratch_shapes=[
            pltpu.VMEM((2, 8, rows), jnp.float32),
            pltpu.VMEM((4, 8, LANES), jnp.float32),
            pltpu.VMEM((2, 8, cols), jnp.float32),
            pltpu.VMEM((2, 8, rows), jnp.float32),
            pltpu.SemaphoreType.DMA((8,)),
            pltpu.SemaphoreType.DMA((8,)),
        ],
        compiler_params=pltpu.CompilerParams(collective_id=1, has_side_effects=True),
        name="diffuse",
    )(acid)


def body(sizes, spectrum, pupil_mask, source_shifts, source_weights):
    pieces, shifts, weights, row_table, col_table, masks = gather(
        spectrum, source_shifts, source_weights, pupil_mask, sizes
    )
    src_count, _, tx_count, ty_count, block_rows, block_cols = pieces.shape
    columns = pieces.reshape(src_count, 2, tx_count * ty_count * block_rows, block_cols)
    acid = image(columns, shifts, weights, row_table, col_table, masks)
    return diffuse(acid, sizes)


def solution(mesh):
    sizes = (mesh.shape["tx"], mesh.shape["ty"], mesh.shape["src"])
    placed = (P(None, ("tx", "ty"), "src"), P(), P("src", None), P("src"))
    return jax.shard_map(
        functools.partial(body, sizes),
        mesh=mesh,
        in_specs=placed,
        out_specs=P(("tx", "src"), "ty"),
        check_vma=False,
    )
```

```python
import functools

import jax
import jax.numpy as jnp
from jax import lax
from jax.experimental import pallas as pl
from jax.experimental.pallas import tpu as pltpu
from jax.sharding import PartitionSpec as P

FRAME = 2048
BY = 256
LANES = 128
GROUP = 4
MESH = pl.DeviceIdType.MESH

diffusion_rate = 0.2


def half_angle(odd, positions):
    turns = (odd * positions) & (2 * FRAME - 1)
    return turns.astype(jnp.float32) * (jnp.pi / FRAME)


def iota(shape, dim):
    return lax.broadcasted_iota(jnp.int32, shape, dim)


def dot(a, b):
    return jnp.dot(a, b, preferred_element_type=jnp.float32)


def reversal(size):
    rows = lax.broadcasted_iota(jnp.int32, (size, size), 0)
    cols = lax.broadcasted_iota(jnp.int32, (size, size), 1)
    return jnp.where(rows + cols == size - 1, 1.0, 0.0).astype(jnp.bfloat16)


def gather_kernel(
    sizes, spec_ref, shift_ref, weight_ref, pupil_ref, all_ref, shifts_ref, weights_ref, row_ref, col_ref, mask_ref,
    send_sem, recv_sem, side_send, side_recv,
):
    tx_count, ty_count, src_count = sizes
    pair_count = tx_count // 2
    tx, t, s = lax.axis_index("tx"), lax.axis_index("ty"), lax.axis_index("src")
    pair, core = tx // 2, lax.rem(tx, 2)
    other_core = 1 - core
    far_t = [lax.rem(t + d, ty_count) for d in range(1, ty_count)]
    far_s = [lax.rem(s + d, src_count) for d in range(1, src_count)]
    far_pair = [lax.rem(pair + d, pair_count) for d in range(1, pair_count)]

    def along_ty(i):
        return {"tx": tx, "ty": i, "src": s}

    def along_src(i):
        return {"tx": tx, "ty": t, "src": i}

    def along_pair(i):
        return {"tx": 2 * i + core, "ty": t, "src": s}

    across = {"tx": 2 * pair + other_core, "ty": t, "src": s}
    partners = [along_ty(i) for i in far_t] + [along_src(i) for i in far_s]
    partners += [along_pair(i) for i in far_pair] + [across]
    barrier = pltpu.get_barrier_semaphore()
    for partner in partners:
        pl.semaphore_signal(barrier, inc=1, device_id=partner, device_id_type=MESH)
    pl.semaphore_wait(barrier, len(partners))

    started = []

    def send(plane, piece, device):
        i, j, k = piece
        slot = all_ref.at[k, plane, i, j]
        own = i is tx and j is t and k is s
        copy = pltpu.make_async_remote_copy(
            src_ref=spec_ref.at[plane] if own else slot,
            dst_ref=slot,
            send_sem=send_sem.at[len(started)],
            recv_sem=recv_sem.at[plane, k, i, j],
            device_id=device,
            device_id_type=MESH,
        )
        copy.start()
        started.append(copy)

    def arrive(plane, piece):
        i, j, k = piece
        slot = all_ref.at[k, plane, i, j]
        pltpu.make_async_remote_copy(
            src_ref=slot,
            dst_ref=slot,
            send_sem=send_sem.at[0],
            recv_sem=recv_sem.at[plane, k, i, j],
            device_id=across,
            device_id_type=MESH,
        ).wait_recv()

    side = []
    for n, i in enumerate(far_s):
        for m, (src, dst) in enumerate(((shift_ref, shifts_ref), (weight_ref, weights_ref))):
            copy = pltpu.make_async_remote_copy(
                src_ref=src,
                dst_ref=dst.at[s],
                send_sem=side_send.at[m, n],
                recv_sem=side_recv.at[m, s],
                device_id=along_src(i),
                device_id_type=MESH,
            )
            copy.start()
            side.append(copy)

    def spread(plane, piece):
        for i in far_s:
            send(plane, piece, along_src(i))
        for i in far_pair:
            send(plane, piece, along_pair(i))
        send(plane, piece, across)

    own = (tx, t, s)
    for plane in range(2):
        for i in far_t:
            send(plane, own, along_ty(i))
    for plane in range(2):
        spread(plane, own)

    shifts_ref[s] = shift_ref[...]
    weights_ref[s] = weight_ref[...]
    for plane in range(2):
        all_ref[s, plane, tx, t] = spec_ref[plane]
    half = pupil_ref.shape[0] // 2
    rows, cols = row_ref.shape[0], col_ref.shape[1]
    x = (tx * src_count + s) * rows + iota((rows, half), 0)
    row_angle = half_angle(2 * iota((rows, half), 1) + 1, x)
    row_ref[:, :half] = jnp.cos(row_angle).astype(jnp.bfloat16)
    row_ref[:, half:] = jnp.sin(row_angle).astype(jnp.bfloat16)
    y = t * cols + iota((half, cols), 1)
    col_angle = half_angle(2 * iota((half, cols), 0) + 1, y)
    col_ref[:half] = jnp.cos(col_angle).astype(jnp.bfloat16)
    col_ref[half:] = jnp.sin(col_angle).astype(jnp.bfloat16)
    small = reversal(half)
    pupil = pupil_ref[...].astype(jnp.float32).astype(jnp.bfloat16)
    mask_ref[0] = pupil[half:, half:].astype(jnp.float32)
    mask_ref[1] = dot(small, pupil[:half, half:])
    mask_ref[2] = dot(pupil[half:, :half], small)
    mask_ref[3] = dot(small, dot(pupil[:half, :half], small).astype(jnp.bfloat16))

    near_first = [t] + far_t
    for j in far_t:
        for plane in range(2):
            arrive(plane, (tx, j, s))
            spread(plane, (tx, j, s))
    for j in near_first:
        for k in far_s:
            arrive(0, (tx, j, k))
            for i in far_pair:
                send(0, (tx, j, k), along_pair(i))
            send(0, (tx, j, k), across)
        for i in far_pair:
            there = 2 * i + core
            arrive(1, (there, j, s))
            for k in far_s:
                send(1, (there, j, s), along_src(k))
            send(1, (there, j, s), across)
        for k in far_s:
            arrive(1, (tx, j, k))
            send(1, (tx, j, k), across)
        for i in far_pair:
            arrive(0, (2 * i + core, j, s))
            send(0, (2 * i + core, j, s), across)
    for j in near_first:
        for i in far_pair:
            for k in far_s:
                for plane in range(2):
                    arrive(plane, (2 * i + core, j, k))
                    send(plane, (2 * i + core, j, k), across)
    for j in near_first:
        for i in [pair] + far_pair:
            for k in [s] + far_s:
                for plane in range(2):
                    arrive(plane, (2 * i + other_core, j, k))
    for n, i in enumerate(far_s):
        for m, (src, dst) in enumerate(((shift_ref, shifts_ref), (weight_ref, weights_ref))):
            pltpu.make_async_remote_copy(
                src_ref=src,
                dst_ref=dst.at[i],
                send_sem=side_send.at[m, n],
                recv_sem=side_recv.at[m, i],
                device_id=across,
                device_id_type=MESH,
            ).wait_recv()
    for copy in started + side:
        copy.wait_send()


def gather(spectrum, source_shifts, source_weights, pupil_mask, sizes):
    tx_count, ty_count, src_count = sizes
    pair_count = tx_count // 2
    _, block_rows, block_cols = spectrum.shape
    slots = source_weights.shape[0]
    half = pupil_mask.shape[0] // 2
    rows = FRAME // (tx_count * src_count)
    vmem = pl.BlockSpec(memory_space=pltpu.VMEM)
    lines = pair_count * src_count * ty_count
    sends = 2 * (ty_count - 1) + 2 * lines + 2 * ty_count * (src_count - 1 + pair_count - 1)
    sends += 2 * ty_count * (src_count - 1) * (pair_count - 1)
    return pl.pallas_call(
        functools.partial(gather_kernel, sizes),
        out_shape=(
            jax.ShapeDtypeStruct((src_count, 2, tx_count, ty_count, block_rows, block_cols), jnp.bfloat16),
            jax.ShapeDtypeStruct((src_count, 2, slots), jnp.int32),
            jax.ShapeDtypeStruct((src_count, 1, slots), jnp.int32),
            jax.ShapeDtypeStruct((rows, 2 * half), jnp.bfloat16),
            jax.ShapeDtypeStruct((2 * half, BY), jnp.bfloat16),
            jax.ShapeDtypeStruct((4, half, half), jnp.float32),
        ),
        in_specs=[vmem] * 4,
        out_specs=(vmem,) * 6,
        scratch_shapes=[
            pltpu.SemaphoreType.DMA((sends,)),
            pltpu.SemaphoreType.DMA((2, src_count, tx_count, ty_count)),
            pltpu.SemaphoreType.DMA((2, src_count)),
            pltpu.SemaphoreType.DMA((2, src_count)),
        ],
        compiler_params=pltpu.CompilerParams(collective_id=0, has_side_effects=True),
        name="gather",
    )(spectrum, source_shifts.T, source_weights[None], pupil_mask)


def image_kernel(
    shifts, weights, spec_ref, masks, row_ref, col_ref, out_ref, flips, acc, folded, inner, live_row, live_col, live_weight
):
    src_count, _, slots = weights.shape
    source_count = src_count * slots
    mask_width = spec_ref.shape[2]
    part = spec_ref.shape[3]
    half = masks.shape[1]
    tiles = mask_width // LANES
    block = 256

    turn = reversal(block)
    for plane in range(2):
        for i in range(mask_width // block):
            for j in range(mask_width // block):
                ri, rj = mask_width // block - 1 - i, mask_width // block - 1 - j
                rows = slice(block * i, block * (i + 1))
                cells = [spec_ref[k, plane, rows] for k in range(block * j // part, -(-block * (j + 1) // part))]
                cell = cells[0] if len(cells) == 1 else jnp.concatenate(cells, axis=1)
                col_flip = dot(cell, turn)
                row_flip = dot(turn, cell)
                both = dot(turn, col_flip.astype(jnp.bfloat16))
                for version, value, vi, vj in (
                    (0, cell.astype(jnp.float32), i, j),
                    (1, row_flip, ri, j),
                    (2, col_flip, i, rj),
                    (3, both, ri, rj),
                ):
                    for t in range(block // LANES):
                        slot = (version * 2 + plane) * tiles + vj * (block // LANES) + t
                        flips[slot, block * vi : block * (vi + 1), :] = value[:, LANES * t : LANES * (t + 1)]

    def pick(i, count):
        group, slot = i // slots, lax.rem(i, slots)
        weight = weights[group, 0, slot]
        live_row[count] = shifts[group, 0, slot]
        live_col[count] = shifts[group, 1, slot]
        live_weight[count + 1] = weight
        return count + (weight > 0).astype(jnp.int32)

    live_weight[0] = 0
    count = lax.fori_loop(0, source_count, pick, jnp.int32(0))
    for g in range(GROUP + 1):
        live_row[count + g] = 0
        live_col[count + g] = 0
        live_weight[count + 1 + g] = 0

    acc[...] = jnp.zeros_like(acc)
    lane = lax.broadcasted_iota(jnp.int32, (half, LANES), 1)

    def fold(a, b, slot):
        row_offsets = (a + half, mask_width - half - a)
        col_offsets = (b + half, mask_width - half - b)
        parts = []
        for plane in range(2):
            quads = []
            for col_side in range(2):
                off = col_offsets[col_side]
                tile, rest = off // LANES, off % LANES
                after = jnp.minimum(tile + 1, tiles - 1)
                back = (LANES - rest) % LANES
                for row_side in range(2):
                    version = 2 * col_side + row_side
                    base = (version * 2 + plane) * tiles
                    rows = pl.ds(row_offsets[row_side], half)
                    left = flips[base + tile, rows, :]
                    right = flips[base + after, rows, :]
                    merged = jnp.where(lane >= rest, left, right)
                    quads.append(pltpu.roll(merged, back, 1) * masks[version])
            s1, d1 = quads[0] + quads[1], quads[0] - quads[1]
            s2, d2 = quads[2] + quads[3], quads[2] - quads[3]
            parts.append((s1, d1, s2, d2))
        (s1, d1, s2, d2), (t1, e1, t2, e2) = parts
        rows = (
            (s1 + s2, t2 - t1),
            (-(e1 + e2), d2 - d1),
            (t1 + t2, s1 - s2),
            (d1 + d2, e2 - e1),
        )
        for n, row in enumerate(rows):
            for m, value in enumerate(row):
                slot[half * n : half * (n + 1), half * m : half * (m + 1)] = value.astype(jnp.bfloat16)

    def step(n, parity):
        fold(live_row[n + 1], live_col[n + 1], folded[1 - parity])
        inner[parity][...] = dot(folded[parity][...], col_ref[...]).astype(jnp.bfloat16)
        weight = live_weight[n].astype(jnp.float32)
        real = dot(row_ref[...], inner[1 - parity][: 2 * half])
        imag = dot(row_ref[...], inner[1 - parity][2 * half :])
        acc[...] += weight * (real * real + imag * imag)

    inner[1][...] = jnp.zeros_like(inner[1])
    fold(live_row[0], live_col[0], folded[0])

    def turn_body(turn_index, carry):
        for g in range(GROUP):
            step(turn_index * GROUP + g, g % 2)
        return carry

    lax.fori_loop(0, (count + GROUP) // GROUP, turn_body, 0)
    out_ref[...] = 1.0 - jnp.exp(-(acc[...] / (2.0 * source_count)))


def image(spectrum, shifts, weights, row_table, col_table, masks):
    source_count = weights.shape[0] * weights.shape[2]
    mask_width = spectrum.shape[2]
    tile = (row_table.shape[0], col_table.shape[1])
    smem = pl.BlockSpec(memory_space=pltpu.SMEM)
    vmem = pl.BlockSpec(memory_space=pltpu.VMEM)
    return pl.pallas_call(
        image_kernel,
        out_shape=jax.ShapeDtypeStruct(tile, jnp.float32),
        in_specs=[smem, smem, vmem, vmem, vmem, vmem],
        out_specs=vmem,
        scratch_shapes=[
            pltpu.VMEM((8 * mask_width // LANES, mask_width, LANES), jnp.float32),
            pltpu.VMEM(tile, jnp.float32),
            [pltpu.VMEM((2 * row_table.shape[1], row_table.shape[1]), jnp.bfloat16)] * 2,
            [pltpu.VMEM((2 * row_table.shape[1], tile[1]), jnp.bfloat16)] * 2,
        ]
        + [pltpu.SMEM((source_count + GROUP + 2,), jnp.int32)] * 3,
        name="image",
    )(shifts, weights, spectrum, masks, row_table, col_table)


def exchange_kernel(sizes, acid_ref, edges, beside, corners, strips, send_sem, recv_sem):
    tx_count, ty_count, src_count = sizes
    rows, cols = acid_ref.shape
    row_block = lax.axis_index("tx") * src_count + lax.axis_index("src")
    col_block = lax.axis_index("ty")
    row_blocks = tx_count * src_count

    def device(dr, dc):
        other = lax.rem(row_block + row_blocks + dr, row_blocks)
        return {
            "tx": other // src_count,
            "src": lax.rem(other, src_count),
            "ty": lax.rem(col_block + ty_count + dc, ty_count),
        }

    around = [(dr, dc) for dr in (-1, 0, 1) for dc in (-1, 0, 1) if (dr, dc) != (0, 0)]
    barrier = pltpu.get_barrier_semaphore()
    for dr, dc in around:
        pl.semaphore_signal(barrier, inc=1, device_id=device(dr, dc), device_id_type=MESH)
    strips[0] = acid_ref[:, :LANES].T[:8]
    strips[1] = acid_ref[:, cols - LANES :].T[LANES - 8 :]
    pl.semaphore_wait(barrier, len(around))

    copies = []
    for n, (dr, dc) in enumerate(around):
        if dc == 0:
            src = acid_ref.at[:8] if dr < 0 else acid_ref.at[rows - 8 :]
            dst = edges.at[0 if dr > 0 else 1]
        elif dr == 0:
            src = strips.at[0 if dc < 0 else 1]
            dst = beside.at[0 if dc > 0 else 1]
        else:
            row_part = slice(0, 8) if dr < 0 else slice(rows - 8, rows)
            col_part = slice(0, LANES) if dc < 0 else slice(cols - LANES, cols)
            src = acid_ref.at[row_part, col_part]
            dst = corners.at[(0 if dr > 0 else 2) + (0 if dc > 0 else 1)]
        copy = pltpu.make_async_remote_copy(
            src_ref=src,
            dst_ref=dst,
            send_sem=send_sem.at[n],
            recv_sem=recv_sem.at[n],
            device_id=device(dr, dc),
            device_id_type=MESH,
        )
        copy.start()
        copies.append(copy)
    for copy in copies:
        copy.wait()


def diffuse_kernel(sizes, acid_ref, edges, beside, corners, out_ref):
    tx_count, ty_count, src_count = sizes
    rows, cols = acid_ref.shape
    none = jnp.zeros((LANES - 8, rows), jnp.float32)
    left = jnp.concatenate([none, beside[0]], axis=0).T
    right = jnp.concatenate([beside[1], none], axis=0).T
    level = jnp.concatenate(
        [
            jnp.concatenate([corners[0], edges[0], corners[1]], axis=1),
            jnp.concatenate([left, acid_ref[...], right], axis=1),
            jnp.concatenate([corners[2], edges[1], corners[3]], axis=1),
        ],
        axis=0,
    )
    row_block = lax.axis_index("tx") * src_count + lax.axis_index("src")
    col_block = lax.axis_index("ty")
    row_blocks = tx_count * src_count
    x = row_block * rows - 8 + lax.broadcasted_iota(jnp.int32, level.shape, 0)
    y = col_block * cols - LANES + lax.broadcasted_iota(jnp.int32, level.shape, 1)
    inside = (x >= 0) & (x < row_blocks * rows) & (y >= 0) & (y < ty_count * cols)
    tall, wide = level.shape
    for repeat in range(2):
        level = jnp.where(inside, level, 0.0)
        near = (
            pltpu.roll(level, 1, 0)
            + pltpu.roll(level, tall - 1, 0)
            + pltpu.roll(level, 1, 1)
            + pltpu.roll(level, wide - 1, 1)
        )
        level = level + diffusion_rate * (near - 4.0 * level)
    out_ref[...] = level[8 : 8 + rows, LANES : LANES + cols]


def diffuse(acid, sizes):
    rows, cols = acid.shape
    vmem = pl.BlockSpec(memory_space=pltpu.VMEM)
    around = pl.pallas_call(
        functools.partial(exchange_kernel, sizes),
        out_shape=(
            jax.ShapeDtypeStruct((2, 8, cols), jnp.float32),
            jax.ShapeDtypeStruct((2, 8, rows), jnp.float32),
            jax.ShapeDtypeStruct((4, 8, LANES), jnp.float32),
        ),
        in_specs=[vmem],
        out_specs=(vmem,) * 3,
        scratch_shapes=[
            pltpu.VMEM((2, 8, rows), jnp.float32),
            pltpu.SemaphoreType.DMA((8,)),
            pltpu.SemaphoreType.DMA((8,)),
        ],
        compiler_params=pltpu.CompilerParams(collective_id=1, has_side_effects=True),
        name="exchange",
    )(acid)
    return pl.pallas_call(
        functools.partial(diffuse_kernel, sizes),
        out_shape=jax.ShapeDtypeStruct((rows, cols), jnp.float32),
        in_specs=[vmem] * 4,
        out_specs=vmem,
        name="diffuse",
    )(acid, *around)


def body(sizes, spectrum, pupil_mask, source_shifts, source_weights):
    pieces, shifts, weights, row_table, col_table, masks = gather(
        spectrum, source_shifts, source_weights, pupil_mask, sizes
    )
    src_count, _, tx_count, ty_count, block_rows, block_cols = pieces.shape
    columns = pieces.reshape(src_count, 2, tx_count * ty_count * block_rows, block_cols)
    acid = image(columns, shifts, weights, row_table, col_table, masks)
    return diffuse(acid, sizes)


def solution(mesh):
    sizes = (mesh.shape["tx"], mesh.shape["ty"], mesh.shape["src"])
    placed = (P(None, ("tx", "ty"), "src"), P(), P("src", None), P("src"))
    return jax.shard_map(
        functools.partial(body, sizes),
        mesh=mesh,
        in_specs=placed,
        out_specs=P(("tx", "src"), "ty"),
        check_vma=False,
    )
```

```python
import functools

import jax
import jax.numpy as jnp
from jax import lax
from jax.experimental import pallas as pl
from jax.experimental.pallas import tpu as pltpu
from jax.sharding import PartitionSpec as P

FRAME = 2048
BY = 256
LANES = 128
GROUP = 4
MESH = pl.DeviceIdType.MESH

diffusion_rate = 0.2


def half_angle(odd, positions):
    turns = (odd * positions) & (2 * FRAME - 1)
    return turns.astype(jnp.float32) * (jnp.pi / FRAME)


def iota(shape, dim):
    return lax.broadcasted_iota(jnp.int32, shape, dim)


def dot(a, b):
    return jnp.dot(a, b, preferred_element_type=jnp.float32)


def reversal(size):
    rows = lax.broadcasted_iota(jnp.int32, (size, size), 0)
    cols = lax.broadcasted_iota(jnp.int32, (size, size), 1)
    return jnp.where(rows + cols == size - 1, 1.0, 0.0).astype(jnp.bfloat16)


def gather_kernel(
    sizes, spec_hbm, shift_ref, weight_ref, pupil_hbm, all_ref, shifts_ref, weights_ref, row_ref, col_ref, mask_ref,
    spec_ref, pupil_ref, local_sem, send_sem, recv_sem, side_send, side_recv,
):
    tx_count, ty_count, src_count = sizes
    pair_count = tx_count // 2
    tx, t, s = lax.axis_index("tx"), lax.axis_index("ty"), lax.axis_index("src")
    pair, core = tx // 2, lax.rem(tx, 2)
    other_core = 1 - core
    far_t = [lax.rem(t + d, ty_count) for d in range(1, ty_count)]
    far_s = [lax.rem(s + d, src_count) for d in range(1, src_count)]
    far_pair = [lax.rem(pair + d, pair_count) for d in range(1, pair_count)]

    def along_ty(i):
        return {"tx": tx, "ty": i, "src": s}

    def along_src(i):
        return {"tx": tx, "ty": t, "src": i}

    def along_pair(i):
        return {"tx": 2 * i + core, "ty": t, "src": s}

    loads = [
        pltpu.make_async_copy(src, dst, local_sem.at[n])
        for n, (src, dst) in enumerate(
            (
                (spec_hbm, spec_ref),
                (pupil_hbm, pupil_ref),
                (shift_ref, shifts_ref.at[s]),
                (weight_ref, weights_ref.at[s]),
            )
        )
    ]
    for load in loads:
        load.start()

    across = {"tx": 2 * pair + other_core, "ty": t, "src": s}
    partners = [along_ty(i) for i in far_t] + [along_src(i) for i in far_s]
    partners += [along_pair(i) for i in far_pair] + [across]
    barrier = pltpu.get_barrier_semaphore()
    for partner in partners:
        pl.semaphore_signal(barrier, inc=1, device_id=partner, device_id_type=MESH)
    pl.semaphore_wait(barrier, len(partners))
    loads[0].wait()

    started = []
    own = (tx, t, s)

    both = slice(None)

    def part(plane, piece):
        i, j, k = piece
        return all_ref.at[k, plane, i, j], recv_sem.at[0 if plane is both else plane, k, i, j]

    def send(plane, piece, device):
        slot, arrived = part(plane, piece)
        copy = pltpu.make_async_remote_copy(
            src_ref=spec_ref if piece is own else slot,
            dst_ref=slot,
            send_sem=send_sem.at[len(started)],
            recv_sem=arrived,
            device_id=device,
            device_id_type=MESH,
        )
        copy.start()
        started.append(copy)

    def arrive(plane, piece):
        slot, arrived = part(plane, piece)
        pltpu.make_async_remote_copy(
            src_ref=slot,
            dst_ref=slot,
            send_sem=send_sem.at[0],
            recv_sem=arrived,
            device_id=across,
            device_id_type=MESH,
        ).wait_recv()

    def spread(piece):
        for i in far_s:
            send(both, piece, along_src(i))
        for i in far_pair:
            send(both, piece, along_pair(i))

    for i in far_t:
        send(both, own, along_ty(i))
    spread(own)
    send(both, own, across)

    side = []
    for n, i in enumerate(far_s):
        for m, (src, dst) in enumerate(((shift_ref, shifts_ref), (weight_ref, weights_ref))):
            copy = pltpu.make_async_remote_copy(
                src_ref=src,
                dst_ref=dst.at[s],
                send_sem=side_send.at[m, n],
                recv_sem=side_recv.at[m, s],
                device_id=along_src(i),
                device_id_type=MESH,
            )
            copy.start()
            side.append(copy)

    for load in loads[1:]:
        load.wait()
    for plane in range(2):
        all_ref[s, plane, tx, t] = spec_ref[plane]
    half = pupil_ref.shape[0] // 2
    rows, cols = row_ref.shape[0], col_ref.shape[1]
    x = (tx * src_count + s) * rows + iota((rows, half), 0)
    row_angle = half_angle(2 * iota((rows, half), 1) + 1, x)
    row_ref[:, :half] = jnp.cos(row_angle).astype(jnp.bfloat16)
    row_ref[:, half:] = jnp.sin(row_angle).astype(jnp.bfloat16)
    y = t * cols + iota((half, cols), 1)
    col_angle = half_angle(2 * iota((half, cols), 0) + 1, y)
    col_ref[:half] = jnp.cos(col_angle).astype(jnp.bfloat16)
    col_ref[half:] = jnp.sin(col_angle).astype(jnp.bfloat16)
    small = reversal(half)
    pupil = pupil_ref[...].astype(jnp.float32).astype(jnp.bfloat16)
    mask_ref[0] = pupil[half:, half:].astype(jnp.float32)
    mask_ref[1] = dot(small, pupil[:half, half:])
    mask_ref[2] = dot(pupil[half:, :half], small)
    mask_ref[3] = dot(small, dot(pupil[:half, :half], small).astype(jnp.bfloat16))

    near_first = [t] + far_t
    for j in far_t:
        arrive(both, (tx, j, s))
        spread((tx, j, s))
    for j in near_first:
        for k in far_s:
            arrive(both, (tx, j, k))
            for i in far_pair:
                send(0, (tx, j, k), along_pair(i))
        for i in far_pair:
            there = 2 * i + core
            arrive(both, (there, j, s))
            for k in far_s:
                send(1, (there, j, s), along_src(k))
        if j is not t:
            send(both, (tx, j, s), across)
        for k in far_s:
            send(both, (tx, j, k), across)
        for i in far_pair:
            send(both, (2 * i + core, j, s), across)
    for j in near_first:
        for i in far_pair:
            for k in far_s:
                for plane in range(2):
                    arrive(plane, (2 * i + core, j, k))
                send(both, (2 * i + core, j, k), across)
    for j in near_first:
        for i in [pair] + far_pair:
            for k in [s] + far_s:
                arrive(both, (2 * i + other_core, j, k))
    for n, i in enumerate(far_s):
        for m, (src, dst) in enumerate(((shift_ref, shifts_ref), (weight_ref, weights_ref))):
            pltpu.make_async_remote_copy(
                src_ref=src,
                dst_ref=dst.at[i],
                send_sem=side_send.at[m, n],
                recv_sem=side_recv.at[m, i],
                device_id=across,
                device_id_type=MESH,
            ).wait_recv()
    for copy in started + side:
        copy.wait_send()


def gather(spectrum, source_shifts, source_weights, pupil_mask, sizes):
    tx_count, ty_count, src_count = sizes
    pair_count = tx_count // 2
    _, block_rows, block_cols = spectrum.shape
    slots = source_weights.shape[0]
    half = pupil_mask.shape[0] // 2
    rows = FRAME // (tx_count * src_count)
    vmem = pl.BlockSpec(memory_space=pltpu.VMEM)
    lines = pair_count * src_count * ty_count
    sends = ty_count - 1 + lines + ty_count * (src_count - 1 + pair_count - 1)
    sends += 2 * ty_count * (src_count - 1) * (pair_count - 1)
    return pl.pallas_call(
        functools.partial(gather_kernel, sizes),
        out_shape=(
            jax.ShapeDtypeStruct((src_count, 2, tx_count, ty_count, block_rows, block_cols), jnp.bfloat16),
            jax.ShapeDtypeStruct((src_count, 2, slots), jnp.int32),
            jax.ShapeDtypeStruct((src_count, 1, slots), jnp.int32),
            jax.ShapeDtypeStruct((rows, 2 * half), jnp.bfloat16),
            jax.ShapeDtypeStruct((2 * half, BY), jnp.bfloat16),
            jax.ShapeDtypeStruct((4, half, half), jnp.float32),
        ),
        in_specs=[pl.BlockSpec(memory_space=pltpu.HBM)] * 4,
        out_specs=(vmem,) * 6,
        scratch_shapes=[
            pltpu.VMEM(spectrum.shape, jnp.bfloat16),
            pltpu.VMEM(pupil_mask.shape, jnp.int32),
            pltpu.SemaphoreType.DMA((4,)),
            pltpu.SemaphoreType.DMA((sends,)),
            pltpu.SemaphoreType.DMA((2, src_count, tx_count, ty_count)),
            pltpu.SemaphoreType.DMA((2, src_count)),
            pltpu.SemaphoreType.DMA((2, src_count)),
        ],
        compiler_params=pltpu.CompilerParams(collective_id=0, has_side_effects=True, vmem_limit_bytes=12 << 20),
        name="gather",
    )(spectrum, source_shifts.T, source_weights[None], pupil_mask)


def image_kernel(
    shifts, weights, spec_ref, masks, row_ref, col_ref, out_ref, flips, acc, folded, inner, live_row, live_col, live_weight
):
    src_count, _, slots = weights.shape
    source_count = src_count * slots
    mask_width = spec_ref.shape[2]
    part = spec_ref.shape[3]
    half = masks.shape[1]
    tiles = mask_width // LANES
    block = 256

    turn = reversal(block)
    for plane in range(2):
        for i in range(mask_width // block):
            for j in range(mask_width // block):
                ri, rj = mask_width // block - 1 - i, mask_width // block - 1 - j
                rows = slice(block * i, block * (i + 1))
                cells = [spec_ref[k, plane, rows] for k in range(block * j // part, -(-block * (j + 1) // part))]
                cell = cells[0] if len(cells) == 1 else jnp.concatenate(cells, axis=1)
                col_flip = dot(cell, turn)
                row_flip = dot(turn, cell)
                both = dot(turn, col_flip.astype(jnp.bfloat16))
                for version, value, vi, vj in (
                    (0, cell.astype(jnp.float32), i, j),
                    (1, row_flip, ri, j),
                    (2, col_flip, i, rj),
                    (3, both, ri, rj),
                ):
                    for t in range(block // LANES):
                        slot = (version * 2 + plane) * tiles + vj * (block // LANES) + t
                        flips[slot, block * vi : block * (vi + 1), :] = value[:, LANES * t : LANES * (t + 1)]

    def pick(i, count):
        group, slot = i // slots, lax.rem(i, slots)
        weight = weights[group, 0, slot]
        live_row[count] = shifts[group, 0, slot]
        live_col[count] = shifts[group, 1, slot]
        live_weight[count + 1] = weight
        return count + (weight > 0).astype(jnp.int32)

    live_weight[0] = 0
    count = lax.fori_loop(0, source_count, pick, jnp.int32(0))
    for g in range(GROUP + 1):
        live_row[count + g] = 0
        live_col[count + g] = 0
        live_weight[count + 1 + g] = 0

    acc[...] = jnp.zeros_like(acc)
    lane = lax.broadcasted_iota(jnp.int32, (half, LANES), 1)

    def fold(a, b, slot):
        row_offsets = (a + half, mask_width - half - a)
        col_offsets = (b + half, mask_width - half - b)
        parts = []
        for plane in range(2):
            quads = []
            for col_side in range(2):
                off = col_offsets[col_side]
                tile, rest = off // LANES, off % LANES
                after = jnp.minimum(tile + 1, tiles - 1)
                back = (LANES - rest) % LANES
                for row_side in range(2):
                    version = 2 * col_side + row_side
                    base = (version * 2 + plane) * tiles
                    rows = pl.ds(row_offsets[row_side], half)
                    left = flips[base + tile, rows, :]
                    right = flips[base + after, rows, :]
                    merged = jnp.where(lane >= rest, left, right)
                    quads.append(pltpu.roll(merged, back, 1) * masks[version])
            s1, d1 = quads[0] + quads[1], quads[0] - quads[1]
            s2, d2 = quads[2] + quads[3], quads[2] - quads[3]
            parts.append((s1, d1, s2, d2))
        (s1, d1, s2, d2), (t1, e1, t2, e2) = parts
        rows = (
            (s1 + s2, t2 - t1),
            (-(e1 + e2), d2 - d1),
            (t1 + t2, s1 - s2),
            (d1 + d2, e2 - e1),
        )
        for n, row in enumerate(rows):
            for m, value in enumerate(row):
                slot[half * n : half * (n + 1), half * m : half * (m + 1)] = value.astype(jnp.bfloat16)

    def step(n, parity):
        fold(live_row[n + 1], live_col[n + 1], folded[1 - parity])
        inner[parity][...] = dot(folded[parity][...], col_ref[...]).astype(jnp.bfloat16)
        weight = live_weight[n].astype(jnp.float32)
        real = dot(row_ref[...], inner[1 - parity][: 2 * half])
        imag = dot(row_ref[...], inner[1 - parity][2 * half :])
        acc[...] += weight * (real * real + imag * imag)

    inner[1][...] = jnp.zeros_like(inner[1])
    fold(live_row[0], live_col[0], folded[0])

    def turn_body(turn_index, carry):
        for g in range(GROUP):
            step(turn_index * GROUP + g, g % 2)
        return carry

    lax.fori_loop(0, (count + GROUP) // GROUP, turn_body, 0)
    out_ref[...] = 1.0 - jnp.exp(-(acc[...] / (2.0 * source_count)))


def image(spectrum, shifts, weights, row_table, col_table, masks):
    source_count = weights.shape[0] * weights.shape[2]
    mask_width = spectrum.shape[2]
    tile = (row_table.shape[0], col_table.shape[1])
    smem = pl.BlockSpec(memory_space=pltpu.SMEM)
    vmem = pl.BlockSpec(memory_space=pltpu.VMEM)
    return pl.pallas_call(
        image_kernel,
        out_shape=jax.ShapeDtypeStruct(tile, jnp.float32),
        in_specs=[smem, smem, vmem, vmem, vmem, vmem],
        out_specs=vmem,
        scratch_shapes=[
            pltpu.VMEM((8 * mask_width // LANES, mask_width, LANES), jnp.float32),
            pltpu.VMEM(tile, jnp.float32),
            [pltpu.VMEM((2 * row_table.shape[1], row_table.shape[1]), jnp.bfloat16)] * 2,
            [pltpu.VMEM((2 * row_table.shape[1], tile[1]), jnp.bfloat16)] * 2,
        ]
        + [pltpu.SMEM((source_count + GROUP + 2,), jnp.int32)] * 3,
        compiler_params=pltpu.CompilerParams(vmem_limit_bytes=28 << 20),
        name="image",
    )(shifts, weights, spectrum, masks, row_table, col_table)


def exchange_kernel(sizes, acid_ref, edges, beside, corners, strips, send_sem, recv_sem):
    tx_count, ty_count, src_count = sizes
    rows, cols = acid_ref.shape
    row_block = lax.axis_index("tx") * src_count + lax.axis_index("src")
    col_block = lax.axis_index("ty")
    row_blocks = tx_count * src_count

    def device(dr, dc):
        other = lax.rem(row_block + row_blocks + dr, row_blocks)
        return {
            "tx": other // src_count,
            "src": lax.rem(other, src_count),
            "ty": lax.rem(col_block + ty_count + dc, ty_count),
        }

    around = [(dr, dc) for dr in (-1, 0, 1) for dc in (-1, 0, 1) if (dr, dc) != (0, 0)]
    barrier = pltpu.get_barrier_semaphore()
    for dr, dc in around:
        pl.semaphore_signal(barrier, inc=1, device_id=device(dr, dc), device_id_type=MESH)
    strips[0] = acid_ref[:, :LANES].T[:8]
    strips[1] = acid_ref[:, cols - LANES :].T[LANES - 8 :]
    pl.semaphore_wait(barrier, len(around))

    copies = []
    for n, (dr, dc) in enumerate(around):
        if dc == 0:
            src = acid_ref.at[:8] if dr < 0 else acid_ref.at[rows - 8 :]
            dst = edges.at[0 if dr > 0 else 1]
        elif dr == 0:
            src = strips.at[0 if dc < 0 else 1]
            dst = beside.at[0 if dc > 0 else 1]
        else:
            row_part = slice(0, 8) if dr < 0 else slice(rows - 8, rows)
            col_part = slice(0, LANES) if dc < 0 else slice(cols - LANES, cols)
            src = acid_ref.at[row_part, col_part]
            dst = corners.at[(0 if dr > 0 else 2) + (0 if dc > 0 else 1)]
        copy = pltpu.make_async_remote_copy(
            src_ref=src,
            dst_ref=dst,
            send_sem=send_sem.at[n],
            recv_sem=recv_sem.at[n],
            device_id=device(dr, dc),
            device_id_type=MESH,
        )
        copy.start()
        copies.append(copy)
    for copy in copies:
        copy.wait()


def diffuse_kernel(sizes, acid_ref, edges, beside, corners, out_ref):
    tx_count, ty_count, src_count = sizes
    rows, cols = acid_ref.shape
    none = jnp.zeros((LANES - 8, rows), jnp.float32)
    left = jnp.concatenate([none, beside[0]], axis=0).T
    right = jnp.concatenate([beside[1], none], axis=0).T
    level = jnp.concatenate(
        [
            jnp.concatenate([corners[0], edges[0], corners[1]], axis=1),
            jnp.concatenate([left, acid_ref[...], right], axis=1),
            jnp.concatenate([corners[2], edges[1], corners[3]], axis=1),
        ],
        axis=0,
    )
    row_block = lax.axis_index("tx") * src_count + lax.axis_index("src")
    col_block = lax.axis_index("ty")
    row_blocks = tx_count * src_count
    x = row_block * rows - 8 + lax.broadcasted_iota(jnp.int32, level.shape, 0)
    y = col_block * cols - LANES + lax.broadcasted_iota(jnp.int32, level.shape, 1)
    inside = (x >= 0) & (x < row_blocks * rows) & (y >= 0) & (y < ty_count * cols)
    tall, wide = level.shape
    for repeat in range(2):
        level = jnp.where(inside, level, 0.0)
        near = (
            pltpu.roll(level, 1, 0)
            + pltpu.roll(level, tall - 1, 0)
            + pltpu.roll(level, 1, 1)
            + pltpu.roll(level, wide - 1, 1)
        )
        level = level + diffusion_rate * (near - 4.0 * level)
    out_ref[...] = level[8 : 8 + rows, LANES : LANES + cols]


def diffuse(acid, sizes):
    rows, cols = acid.shape
    vmem = pl.BlockSpec(memory_space=pltpu.VMEM)
    around = pl.pallas_call(
        functools.partial(exchange_kernel, sizes),
        out_shape=(
            jax.ShapeDtypeStruct((2, 8, cols), jnp.float32),
            jax.ShapeDtypeStruct((2, 8, rows), jnp.float32),
            jax.ShapeDtypeStruct((4, 8, LANES), jnp.float32),
        ),
        in_specs=[vmem],
        out_specs=(vmem,) * 3,
        scratch_shapes=[
            pltpu.VMEM((2, 8, rows), jnp.float32),
            pltpu.SemaphoreType.DMA((8,)),
            pltpu.SemaphoreType.DMA((8,)),
        ],
        compiler_params=pltpu.CompilerParams(collective_id=1, has_side_effects=True, vmem_limit_bytes=4 << 20),
        name="exchange",
    )(acid)
    return pl.pallas_call(
        functools.partial(diffuse_kernel, sizes),
        out_shape=jax.ShapeDtypeStruct((rows, cols), jnp.float32),
        in_specs=[vmem] * 4,
        out_specs=vmem,
        compiler_params=pltpu.CompilerParams(vmem_limit_bytes=12 << 20),
        name="diffuse",
    )(acid, *around)


def body(sizes, spectrum, pupil_mask, source_shifts, source_weights):
    pieces, shifts, weights, row_table, col_table, masks = gather(
        spectrum, source_shifts, source_weights, pupil_mask, sizes
    )
    src_count, _, tx_count, ty_count, block_rows, block_cols = pieces.shape
    columns = pieces.reshape(src_count, 2, tx_count * ty_count * block_rows, block_cols)
    acid = image(columns, shifts, weights, row_table, col_table, masks)
    return diffuse(acid, sizes)


def solution(mesh):
    sizes = (mesh.shape["tx"], mesh.shape["ty"], mesh.shape["src"])
    placed = (P(None, ("tx", "ty"), "src"), P(), P("src", None), P("src"))
    return jax.shard_map(
        functools.partial(body, sizes),
        mesh=mesh,
        in_specs=placed,
        out_specs=P(("tx", "src"), "ty"),
        check_vma=False,
    )
```

```python
import functools

import jax
import jax.numpy as jnp
from jax import lax
from jax.experimental import pallas as pl
from jax.experimental.pallas import tpu as pltpu
from jax.sharding import PartitionSpec as P

FRAME = 2048
BY = 256
LANES = 128
GROUP = 4
MESH = pl.DeviceIdType.MESH

diffusion_rate = 0.2


def half_angle(odd, positions):
    turns = (odd * positions) & (2 * FRAME - 1)
    return turns.astype(jnp.float32) * (jnp.pi / FRAME)


def iota(shape, dim):
    return lax.broadcasted_iota(jnp.int32, shape, dim)


def dot(a, b):
    return jnp.dot(a, b, preferred_element_type=jnp.float32)


def reversal(size):
    rows = lax.broadcasted_iota(jnp.int32, (size, size), 0)
    cols = lax.broadcasted_iota(jnp.int32, (size, size), 1)
    return jnp.where(rows + cols == size - 1, 1.0, 0.0).astype(jnp.bfloat16)


def flip_bits(index, mask):
    bit = 1
    while bit <= mask:
        if mask & bit:
            index = index + bit * (1 - 2 * lax.rem(index // bit, 2))
        bit *= 2
    return index


def others(index, count):
    if count & (count - 1) == 0:
        return [flip_bits(index, d) for d in range(1, count)]
    return [lax.rem(index + d, count) for d in range(1, count)]


def gather_kernel(
    sizes, spec_hbm, shift_ref, weight_ref, pupil_hbm, all_ref, shifts_ref, weights_ref, row_ref, col_ref, mask_ref,
    spec_ref, pupil_ref, local_sem, send_sem, recv_sem, side_send, side_recv,
):
    tx_count, ty_count, src_count = sizes
    pair_count = tx_count // 2
    tx, t, s = lax.axis_index("tx"), lax.axis_index("ty"), lax.axis_index("src")
    pair, core = tx // 2, lax.rem(tx, 2)
    other_core = 1 - core
    far_t = others(t, ty_count)
    far_s = others(s, src_count)
    far_pair = others(pair, pair_count)

    def along_ty(i):
        return {"tx": tx, "ty": i, "src": s}

    def along_src(i):
        return {"tx": tx, "ty": t, "src": i}

    def along_pair(i):
        return {"tx": 2 * i + core, "ty": t, "src": s}

    loads = [
        pltpu.make_async_copy(src, dst, local_sem.at[n])
        for n, (src, dst) in enumerate(
            (
                (spec_hbm, spec_ref),
                (pupil_hbm, pupil_ref),
                (shift_ref, shifts_ref.at[s]),
                (weight_ref, weights_ref.at[s]),
            )
        )
    ]
    for load in loads:
        load.start()

    across = {"tx": 2 * pair + other_core, "ty": t, "src": s}
    partners = [along_ty(i) for i in far_t] + [along_src(i) for i in far_s]
    partners += [along_pair(i) for i in far_pair] + [across]
    barrier = pltpu.get_barrier_semaphore()
    for partner in partners:
        pl.semaphore_signal(barrier, inc=1, device_id=partner, device_id_type=MESH)
    pl.semaphore_wait(barrier, len(partners))
    loads[0].wait()

    started = []
    own = (tx, t, s)

    both = slice(None)

    def part(plane, piece):
        i, j, k = piece
        return all_ref.at[k, plane, i, j], recv_sem.at[0 if plane is both else plane, k, i, j]

    def send(plane, piece, device):
        slot, arrived = part(plane, piece)
        copy = pltpu.make_async_remote_copy(
            src_ref=spec_ref if piece is own else slot,
            dst_ref=slot,
            send_sem=send_sem.at[len(started)],
            recv_sem=arrived,
            device_id=device,
            device_id_type=MESH,
        )
        copy.start()
        started.append(copy)

    def arrive(plane, piece):
        slot, arrived = part(plane, piece)
        pltpu.make_async_remote_copy(
            src_ref=slot,
            dst_ref=slot,
            send_sem=send_sem.at[0],
            recv_sem=arrived,
            device_id=across,
            device_id_type=MESH,
        ).wait_recv()

    def spread(piece):
        for i in far_s:
            send(both, piece, along_src(i))
        for i in far_pair:
            send(both, piece, along_pair(i))

    for i in far_t:
        send(both, own, along_ty(i))
    spread(own)
    send(both, own, across)

    side = []
    for n, i in enumerate(far_s):
        for m, (src, dst) in enumerate(((shift_ref, shifts_ref), (weight_ref, weights_ref))):
            copy = pltpu.make_async_remote_copy(
                src_ref=src,
                dst_ref=dst.at[s],
                send_sem=side_send.at[m, n],
                recv_sem=side_recv.at[m, s],
                device_id=along_src(i),
                device_id_type=MESH,
            )
            copy.start()
            side.append(copy)

    for load in loads[1:]:
        load.wait()
    for plane in range(2):
        all_ref[s, plane, tx, t] = spec_ref[plane]
    half = pupil_ref.shape[0] // 2
    rows, cols = row_ref.shape[0], col_ref.shape[1]
    x = (tx * src_count + s) * rows + iota((rows, half), 0)
    row_angle = half_angle(2 * iota((rows, half), 1) + 1, x)
    row_ref[:, :half] = jnp.cos(row_angle).astype(jnp.bfloat16)
    row_ref[:, half:] = jnp.sin(row_angle).astype(jnp.bfloat16)
    y = t * cols + iota((half, cols), 1)
    col_angle = half_angle(2 * iota((half, cols), 0) + 1, y)
    col_ref[:half] = jnp.cos(col_angle).astype(jnp.bfloat16)
    col_ref[half:] = jnp.sin(col_angle).astype(jnp.bfloat16)
    small = reversal(half)
    pupil = pupil_ref[...].astype(jnp.float32).astype(jnp.bfloat16)
    mask_ref[0] = pupil[half:, half:].astype(jnp.float32)
    mask_ref[1] = dot(small, pupil[:half, half:])
    mask_ref[2] = dot(pupil[half:, :half], small)
    mask_ref[3] = dot(small, dot(pupil[:half, :half], small).astype(jnp.bfloat16))

    near_first = [t] + far_t
    for j in far_t:
        arrive(both, (tx, j, s))
        spread((tx, j, s))
    for j in near_first:
        for k in far_s:
            arrive(both, (tx, j, k))
            for i in far_pair:
                send(0, (tx, j, k), along_pair(i))
        for i in far_pair:
            there = 2 * i + core
            arrive(both, (there, j, s))
            for k in far_s:
                send(1, (there, j, s), along_src(k))
        if j is not t:
            send(both, (tx, j, s), across)
        for k in far_s:
            send(both, (tx, j, k), across)
        for i in far_pair:
            send(both, (2 * i + core, j, s), across)
    for j in near_first:
        for i in far_pair:
            for k in far_s:
                for plane in range(2):
                    arrive(plane, (2 * i + core, j, k))
                send(both, (2 * i + core, j, k), across)
    for j in near_first:
        for i in [pair] + far_pair:
            for k in [s] + far_s:
                arrive(both, (2 * i + other_core, j, k))
    for n, i in enumerate(far_s):
        for m, (src, dst) in enumerate(((shift_ref, shifts_ref), (weight_ref, weights_ref))):
            pltpu.make_async_remote_copy(
                src_ref=src,
                dst_ref=dst.at[i],
                send_sem=side_send.at[m, n],
                recv_sem=side_recv.at[m, i],
                device_id=across,
                device_id_type=MESH,
            ).wait_recv()
    for copy in started + side:
        copy.wait_send()


def gather(spectrum, source_shifts, source_weights, pupil_mask, sizes):
    tx_count, ty_count, src_count = sizes
    pair_count = tx_count // 2
    _, block_rows, block_cols = spectrum.shape
    slots = source_weights.shape[0]
    half = pupil_mask.shape[0] // 2
    rows = FRAME // (tx_count * src_count)
    vmem = pl.BlockSpec(memory_space=pltpu.VMEM)
    lines = pair_count * src_count * ty_count
    sends = ty_count - 1 + lines + ty_count * (src_count - 1 + pair_count - 1)
    sends += 2 * ty_count * (src_count - 1) * (pair_count - 1)
    return pl.pallas_call(
        functools.partial(gather_kernel, sizes),
        out_shape=(
            jax.ShapeDtypeStruct((src_count, 2, tx_count, ty_count, block_rows, block_cols), jnp.bfloat16),
            jax.ShapeDtypeStruct((src_count, 2, slots), jnp.int32),
            jax.ShapeDtypeStruct((src_count, 1, slots), jnp.int32),
            jax.ShapeDtypeStruct((rows, 2 * half), jnp.bfloat16),
            jax.ShapeDtypeStruct((2 * half, BY), jnp.bfloat16),
            jax.ShapeDtypeStruct((4, half, half), jnp.float32),
        ),
        in_specs=[pl.BlockSpec(memory_space=pltpu.HBM)] * 4,
        out_specs=(vmem,) * 6,
        scratch_shapes=[
            pltpu.VMEM(spectrum.shape, jnp.bfloat16),
            pltpu.VMEM(pupil_mask.shape, jnp.int32),
            pltpu.SemaphoreType.DMA((4,)),
            pltpu.SemaphoreType.DMA((sends,)),
            pltpu.SemaphoreType.DMA((2, src_count, tx_count, ty_count)),
            pltpu.SemaphoreType.DMA((2, src_count)),
            pltpu.SemaphoreType.DMA((2, src_count)),
        ],
        compiler_params=pltpu.CompilerParams(collective_id=0, has_side_effects=True, vmem_limit_bytes=12 << 20),
        name="gather",
    )(*(pltpu.with_memory_space_constraint(a, pltpu.HBM) for a in (spectrum, source_shifts.T, source_weights[None], pupil_mask)))


def image_kernel(
    shifts, weights, spec_ref, masks, row_ref, col_ref, out_ref, flips, acc, folded, inner, live_row, live_col, live_weight
):
    src_count, _, slots = weights.shape
    source_count = src_count * slots
    mask_width = spec_ref.shape[2]
    part = spec_ref.shape[3]
    half = masks.shape[1]
    tiles = mask_width // LANES
    block = 256

    turn = reversal(block)
    for plane in range(2):
        for i in range(mask_width // block):
            for j in range(mask_width // block):
                ri, rj = mask_width // block - 1 - i, mask_width // block - 1 - j
                rows = slice(block * i, block * (i + 1))
                cells = [spec_ref[k, plane, rows] for k in range(block * j // part, -(-block * (j + 1) // part))]
                cell = cells[0] if len(cells) == 1 else jnp.concatenate(cells, axis=1)
                col_flip = dot(cell, turn)
                row_flip = dot(turn, cell)
                both = dot(turn, col_flip.astype(jnp.bfloat16))
                for version, value, vi, vj in (
                    (0, cell.astype(jnp.float32), i, j),
                    (1, row_flip, ri, j),
                    (2, col_flip, i, rj),
                    (3, both, ri, rj),
                ):
                    for t in range(block // LANES):
                        slot = (version * 2 + plane) * tiles + vj * (block // LANES) + t
                        flips[slot, block * vi : block * (vi + 1), :] = value[:, LANES * t : LANES * (t + 1)]

    def pick(i, count):
        group, slot = i // slots, lax.rem(i, slots)
        weight = weights[group, 0, slot]
        live_row[count] = shifts[group, 0, slot]
        live_col[count] = shifts[group, 1, slot]
        live_weight[count + 1] = weight
        return count + (weight > 0).astype(jnp.int32)

    live_weight[0] = 0
    count = lax.fori_loop(0, source_count, pick, jnp.int32(0))
    for g in range(GROUP + 1):
        live_row[count + g] = 0
        live_col[count + g] = 0
        live_weight[count + 1 + g] = 0

    acc[...] = jnp.zeros_like(acc)
    lane = lax.broadcasted_iota(jnp.int32, (half, LANES), 1)

    def fold(a, b, slot):
        row_offsets = (a + half, mask_width - half - a)
        col_offsets = (b + half, mask_width - half - b)
        parts = []
        for plane in range(2):
            quads = []
            for col_side in range(2):
                off = col_offsets[col_side]
                tile, rest = off // LANES, off % LANES
                after = jnp.minimum(tile + 1, tiles - 1)
                back = (LANES - rest) % LANES
                for row_side in range(2):
                    version = 2 * col_side + row_side
                    base = (version * 2 + plane) * tiles
                    rows = pl.ds(row_offsets[row_side], half)
                    left = flips[base + tile, rows, :]
                    right = flips[base + after, rows, :]
                    merged = jnp.where(lane >= rest, left, right)
                    quads.append(pltpu.roll(merged, back, 1) * masks[version])
            s1, d1 = quads[0] + quads[1], quads[0] - quads[1]
            s2, d2 = quads[2] + quads[3], quads[2] - quads[3]
            parts.append((s1, d1, s2, d2))
        (s1, d1, s2, d2), (t1, e1, t2, e2) = parts
        rows = (
            (s1 + s2, t2 - t1),
            (-(e1 + e2), d2 - d1),
            (t1 + t2, s1 - s2),
            (d1 + d2, e2 - e1),
        )
        for n, row in enumerate(rows):
            for m, value in enumerate(row):
                slot[half * n : half * (n + 1), half * m : half * (m + 1)] = value.astype(jnp.bfloat16)

    def step(n, parity):
        fold(live_row[n + 1], live_col[n + 1], folded[1 - parity])
        inner[parity][...] = dot(folded[parity][...], col_ref[...]).astype(jnp.bfloat16)
        weight = live_weight[n].astype(jnp.float32)
        real = dot(row_ref[...], inner[1 - parity][: 2 * half])
        imag = dot(row_ref[...], inner[1 - parity][2 * half :])
        acc[...] += weight * (real * real + imag * imag)

    inner[1][...] = jnp.zeros_like(inner[1])
    fold(live_row[0], live_col[0], folded[0])

    def turn_body(turn_index, carry):
        for g in range(GROUP):
            step(turn_index * GROUP + g, g % 2)
        return carry

    lax.fori_loop(0, (count + GROUP) // GROUP, turn_body, 0)
    out_ref[...] = 1.0 - jnp.exp(-(acc[...] / (2.0 * source_count)))


def image(spectrum, shifts, weights, row_table, col_table, masks):
    source_count = weights.shape[0] * weights.shape[2]
    mask_width = spectrum.shape[2]
    tile = (row_table.shape[0], col_table.shape[1])
    smem = pl.BlockSpec(memory_space=pltpu.SMEM)
    vmem = pl.BlockSpec(memory_space=pltpu.VMEM)
    return pl.pallas_call(
        image_kernel,
        out_shape=jax.ShapeDtypeStruct(tile, jnp.float32),
        in_specs=[smem, smem, vmem, vmem, vmem, vmem],
        out_specs=vmem,
        scratch_shapes=[
            pltpu.VMEM((8 * mask_width // LANES, mask_width, LANES), jnp.float32),
            pltpu.VMEM(tile, jnp.float32),
            [pltpu.VMEM((2 * row_table.shape[1], row_table.shape[1]), jnp.bfloat16)] * 2,
            [pltpu.VMEM((2 * row_table.shape[1], tile[1]), jnp.bfloat16)] * 2,
        ]
        + [pltpu.SMEM((source_count + GROUP + 2,), jnp.int32)] * 3,
        compiler_params=pltpu.CompilerParams(vmem_limit_bytes=28 << 20),
        name="image",
    )(shifts, weights, spectrum, masks, row_table, col_table)


def exchange_kernel(sizes, acid_ref, edges, beside, corners, strips, send_sem, recv_sem):
    tx_count, ty_count, src_count = sizes
    rows, cols = acid_ref.shape
    row_block = lax.axis_index("tx") * src_count + lax.axis_index("src")
    col_block = lax.axis_index("ty")
    row_blocks = tx_count * src_count

    def device(dr, dc):
        other = lax.rem(row_block + row_blocks + dr, row_blocks)
        return {
            "tx": other // src_count,
            "src": lax.rem(other, src_count),
            "ty": lax.rem(col_block + ty_count + dc, ty_count),
        }

    around = [(dr, dc) for dr in (-1, 0, 1) for dc in (-1, 0, 1) if (dr, dc) != (0, 0)]
    barrier = pltpu.get_barrier_semaphore()
    for dr, dc in around:
        pl.semaphore_signal(barrier, inc=1, device_id=device(dr, dc), device_id_type=MESH)
    strips[0] = acid_ref[:, :LANES].T[:8]
    strips[1] = acid_ref[:, cols - LANES :].T[LANES - 8 :]
    pl.semaphore_wait(barrier, len(around))

    copies = []
    for n, (dr, dc) in enumerate(around):
        if dc == 0:
            src = acid_ref.at[:8] if dr < 0 else acid_ref.at[rows - 8 :]
            dst = edges.at[0 if dr > 0 else 1]
        elif dr == 0:
            src = strips.at[0 if dc < 0 else 1]
            dst = beside.at[0 if dc > 0 else 1]
        else:
            row_part = slice(0, 8) if dr < 0 else slice(rows - 8, rows)
            col_part = slice(0, LANES) if dc < 0 else slice(cols - LANES, cols)
            src = acid_ref.at[row_part, col_part]
            dst = corners.at[(0 if dr > 0 else 2) + (0 if dc > 0 else 1)]
        copy = pltpu.make_async_remote_copy(
            src_ref=src,
            dst_ref=dst,
            send_sem=send_sem.at[n],
            recv_sem=recv_sem.at[n],
            device_id=device(dr, dc),
            device_id_type=MESH,
        )
        copy.start()
        copies.append(copy)
    for copy in copies:
        copy.wait()


def diffuse_kernel(sizes, acid_ref, edges, beside, corners, out_ref):
    tx_count, ty_count, src_count = sizes
    rows, cols = acid_ref.shape
    none = jnp.zeros((LANES - 8, rows), jnp.float32)
    left = jnp.concatenate([none, beside[0]], axis=0).T
    right = jnp.concatenate([beside[1], none], axis=0).T
    level = jnp.concatenate(
        [
            jnp.concatenate([corners[0], edges[0], corners[1]], axis=1),
            jnp.concatenate([left, acid_ref[...], right], axis=1),
            jnp.concatenate([corners[2], edges[1], corners[3]], axis=1),
        ],
        axis=0,
    )
    row_block = lax.axis_index("tx") * src_count + lax.axis_index("src")
    col_block = lax.axis_index("ty")
    row_blocks = tx_count * src_count
    x = row_block * rows - 8 + lax.broadcasted_iota(jnp.int32, level.shape, 0)
    y = col_block * cols - LANES + lax.broadcasted_iota(jnp.int32, level.shape, 1)
    inside = (x >= 0) & (x < row_blocks * rows) & (y >= 0) & (y < ty_count * cols)
    tall, wide = level.shape
    for repeat in range(2):
        level = jnp.where(inside, level, 0.0)
        near = (
            pltpu.roll(level, 1, 0)
            + pltpu.roll(level, tall - 1, 0)
            + pltpu.roll(level, 1, 1)
            + pltpu.roll(level, wide - 1, 1)
        )
        level = level + diffusion_rate * (near - 4.0 * level)
    out_ref[...] = level[8 : 8 + rows, LANES : LANES + cols]


def diffuse(acid, sizes):
    rows, cols = acid.shape
    vmem = pl.BlockSpec(memory_space=pltpu.VMEM)
    around = pl.pallas_call(
        functools.partial(exchange_kernel, sizes),
        out_shape=(
            jax.ShapeDtypeStruct((2, 8, cols), jnp.float32),
            jax.ShapeDtypeStruct((2, 8, rows), jnp.float32),
            jax.ShapeDtypeStruct((4, 8, LANES), jnp.float32),
        ),
        in_specs=[vmem],
        out_specs=(vmem,) * 3,
        scratch_shapes=[
            pltpu.VMEM((2, 8, rows), jnp.float32),
            pltpu.SemaphoreType.DMA((8,)),
            pltpu.SemaphoreType.DMA((8,)),
        ],
        compiler_params=pltpu.CompilerParams(collective_id=1, has_side_effects=True, vmem_limit_bytes=4 << 20),
        name="exchange",
    )(acid)
    return pl.pallas_call(
        functools.partial(diffuse_kernel, sizes),
        out_shape=jax.ShapeDtypeStruct((rows, cols), jnp.float32),
        in_specs=[vmem] * 4,
        out_specs=vmem,
        compiler_params=pltpu.CompilerParams(vmem_limit_bytes=12 << 20),
        name="diffuse",
    )(acid, *around)


def body(sizes, spectrum, pupil_mask, source_shifts, source_weights):
    pieces, shifts, weights, row_table, col_table, masks = gather(
        spectrum, source_shifts, source_weights, pupil_mask, sizes
    )
    src_count, _, tx_count, ty_count, block_rows, block_cols = pieces.shape
    columns = pieces.reshape(src_count, 2, tx_count * ty_count * block_rows, block_cols)
    acid = image(columns, shifts, weights, row_table, col_table, masks)
    return diffuse(acid, sizes)


def solution(mesh):
    sizes = (mesh.shape["tx"], mesh.shape["ty"], mesh.shape["src"])
    placed = (P(None, ("tx", "ty"), "src"), P(), P("src", None), P("src"))
    return jax.shard_map(
        functools.partial(body, sizes),
        mesh=mesh,
        in_specs=placed,
        out_specs=P(("tx", "src"), "ty"),
        check_vma=False,
    )
```

```python
import functools

import jax
import jax.numpy as jnp
from jax import lax
from jax.experimental import pallas as pl
from jax.experimental.pallas import tpu as pltpu
from jax.sharding import PartitionSpec as P

FRAME = 2048
BY = 256
LANES = 128
GROUP = 6
MESH = pl.DeviceIdType.MESH

diffusion_rate = 0.2


def half_angle(odd, positions):
    turns = (odd * positions) & (2 * FRAME - 1)
    return turns.astype(jnp.float32) * (jnp.pi / FRAME)


def iota(shape, dim):
    return lax.broadcasted_iota(jnp.int32, shape, dim)


def dot(a, b):
    return jnp.dot(a, b, preferred_element_type=jnp.float32)


def reversal(size):
    rows = lax.broadcasted_iota(jnp.int32, (size, size), 0)
    cols = lax.broadcasted_iota(jnp.int32, (size, size), 1)
    return jnp.where(rows + cols == size - 1, 1.0, 0.0).astype(jnp.bfloat16)


def flip_bits(index, mask):
    bit = 1
    while bit <= mask:
        if mask & bit:
            index = index + bit * (1 - 2 * lax.rem(index // bit, 2))
        bit *= 2
    return index


def others(index, count):
    if count & (count - 1) == 0:
        return [flip_bits(index, d) for d in range(1, count)]
    return [lax.rem(index + d, count) for d in range(1, count)]


def gather_kernel(
    sizes, spec_hbm, shift_ref, weight_ref, pupil_hbm, all_ref, shifts_ref, weights_ref, row_ref, col_ref, mask_ref,
    spec_ref, pupil_ref, local_sem, send_sem, recv_sem, side_send, side_recv,
):
    tx_count, ty_count, src_count = sizes
    pair_count = tx_count // 2
    tx, t, s = lax.axis_index("tx"), lax.axis_index("ty"), lax.axis_index("src")
    pair, core = tx // 2, lax.rem(tx, 2)
    other_core = 1 - core
    far_t = others(t, ty_count)
    far_s = others(s, src_count)
    far_pair = others(pair, pair_count)

    def along_ty(i):
        return {"tx": tx, "ty": i, "src": s}

    def along_src(i):
        return {"tx": tx, "ty": t, "src": i}

    def along_pair(i):
        return {"tx": 2 * i + core, "ty": t, "src": s}

    loads = [
        pltpu.make_async_copy(src, dst, local_sem.at[n])
        for n, (src, dst) in enumerate(
            (
                (spec_hbm, spec_ref),
                (pupil_hbm, pupil_ref),
                (shift_ref, shifts_ref.at[s]),
                (weight_ref, weights_ref.at[s]),
            )
        )
    ]
    for load in loads:
        load.start()

    across = {"tx": 2 * pair + other_core, "ty": t, "src": s}
    partners = [along_ty(i) for i in far_t] + [along_src(i) for i in far_s]
    partners += [along_pair(i) for i in far_pair] + [across]
    barrier = pltpu.get_barrier_semaphore()
    for partner in partners:
        pl.semaphore_signal(barrier, inc=1, device_id=partner, device_id_type=MESH)
    pl.semaphore_wait(barrier, len(partners))
    loads[0].wait()

    started = []
    own = (tx, t, s)

    both = slice(None)

    def part(plane, piece):
        i, j, k = piece
        return all_ref.at[k, plane, i, j], recv_sem.at[0 if plane is both else plane, k, i, j]

    def send(plane, piece, device):
        slot, arrived = part(plane, piece)
        copy = pltpu.make_async_remote_copy(
            src_ref=spec_ref if piece is own else slot,
            dst_ref=slot,
            send_sem=send_sem.at[len(started)],
            recv_sem=arrived,
            device_id=device,
            device_id_type=MESH,
        )
        copy.start()
        started.append(copy)

    def arrive(plane, piece):
        slot, arrived = part(plane, piece)
        pltpu.make_async_remote_copy(
            src_ref=slot,
            dst_ref=slot,
            send_sem=send_sem.at[0],
            recv_sem=arrived,
            device_id=across,
            device_id_type=MESH,
        ).wait_recv()

    def spread(piece):
        for i in far_s:
            send(both, piece, along_src(i))
        for i in far_pair:
            send(both, piece, along_pair(i))

    for i in far_t:
        send(both, own, along_ty(i))
    spread(own)
    send(both, own, across)

    side = []
    for n, i in enumerate(far_s):
        for m, (src, dst) in enumerate(((shift_ref, shifts_ref), (weight_ref, weights_ref))):
            copy = pltpu.make_async_remote_copy(
                src_ref=src,
                dst_ref=dst.at[s],
                send_sem=side_send.at[m, n],
                recv_sem=side_recv.at[m, s],
                device_id=along_src(i),
                device_id_type=MESH,
            )
            copy.start()
            side.append(copy)

    for load in loads[1:]:
        load.wait()
    for plane in range(2):
        all_ref[s, plane, tx, t] = spec_ref[plane]
    half = pupil_ref.shape[0] // 2
    rows, cols = row_ref.shape[0], col_ref.shape[1]
    x = (tx * src_count + s) * rows + iota((rows, half), 0)
    row_angle = half_angle(2 * iota((rows, half), 1) + 1, x)
    row_ref[:, :half] = jnp.cos(row_angle).astype(jnp.bfloat16)
    row_ref[:, half:] = jnp.sin(row_angle).astype(jnp.bfloat16)
    y = t * cols + iota((half, cols), 1)
    col_angle = half_angle(2 * iota((half, cols), 0) + 1, y)
    col_ref[:half] = jnp.cos(col_angle).astype(jnp.bfloat16)
    col_ref[half:] = jnp.sin(col_angle).astype(jnp.bfloat16)
    small = reversal(half)
    pupil = pupil_ref[...].astype(jnp.float32).astype(jnp.bfloat16)
    mask_ref[0] = pupil[half:, half:].astype(jnp.float32)
    mask_ref[1] = dot(small, pupil[:half, half:])
    mask_ref[2] = dot(pupil[half:, :half], small)
    mask_ref[3] = dot(small, dot(pupil[:half, :half], small).astype(jnp.bfloat16))

    near_first = [t] + far_t
    for j in far_t:
        arrive(both, (tx, j, s))
        spread((tx, j, s))
    for j in near_first:
        for k in far_s:
            arrive(both, (tx, j, k))
            for i in far_pair:
                send(0, (tx, j, k), along_pair(i))
        for i in far_pair:
            there = 2 * i + core
            arrive(both, (there, j, s))
            for k in far_s:
                send(1, (there, j, s), along_src(k))
        if j is not t:
            send(both, (tx, j, s), across)
        for k in far_s:
            send(both, (tx, j, k), across)
        for i in far_pair:
            send(both, (2 * i + core, j, s), across)
    for j in near_first:
        for i in far_pair:
            for k in far_s:
                for plane in range(2):
                    arrive(plane, (2 * i + core, j, k))
                send(both, (2 * i + core, j, k), across)
    for j in near_first:
        for i in [pair] + far_pair:
            for k in [s] + far_s:
                arrive(both, (2 * i + other_core, j, k))
    for n, i in enumerate(far_s):
        for m, (src, dst) in enumerate(((shift_ref, shifts_ref), (weight_ref, weights_ref))):
            pltpu.make_async_remote_copy(
                src_ref=src,
                dst_ref=dst.at[i],
                send_sem=side_send.at[m, n],
                recv_sem=side_recv.at[m, i],
                device_id=across,
                device_id_type=MESH,
            ).wait_recv()
    for copy in started + side:
        copy.wait_send()


def gather(spectrum, source_shifts, source_weights, pupil_mask, sizes):
    tx_count, ty_count, src_count = sizes
    pair_count = tx_count // 2
    _, block_rows, block_cols = spectrum.shape
    slots = source_weights.shape[0]
    half = pupil_mask.shape[0] // 2
    rows = FRAME // (tx_count * src_count)
    vmem = pl.BlockSpec(memory_space=pltpu.VMEM)
    lines = pair_count * src_count * ty_count
    sends = ty_count - 1 + lines + ty_count * (src_count - 1 + pair_count - 1)
    sends += 2 * ty_count * (src_count - 1) * (pair_count - 1)
    return pl.pallas_call(
        functools.partial(gather_kernel, sizes),
        out_shape=(
            jax.ShapeDtypeStruct((src_count, 2, tx_count, ty_count, block_rows, block_cols), jnp.bfloat16),
            jax.ShapeDtypeStruct((src_count, 2, slots), jnp.int32),
            jax.ShapeDtypeStruct((src_count, 1, slots), jnp.int32),
            jax.ShapeDtypeStruct((rows, 2 * half), jnp.bfloat16),
            jax.ShapeDtypeStruct((2 * half, BY), jnp.bfloat16),
            jax.ShapeDtypeStruct((4, half, half), jnp.float32),
        ),
        in_specs=[pl.BlockSpec(memory_space=pltpu.HBM)] * 4,
        out_specs=(vmem,) * 6,
        scratch_shapes=[
            pltpu.VMEM(spectrum.shape, jnp.bfloat16),
            pltpu.VMEM(pupil_mask.shape, jnp.int32),
            pltpu.SemaphoreType.DMA((4,)),
            pltpu.SemaphoreType.DMA((sends,)),
            pltpu.SemaphoreType.DMA((2, src_count, tx_count, ty_count)),
            pltpu.SemaphoreType.DMA((2, src_count)),
            pltpu.SemaphoreType.DMA((2, src_count)),
        ],
        compiler_params=pltpu.CompilerParams(collective_id=0, has_side_effects=True, vmem_limit_bytes=12 << 20),
        name="gather",
    )(*(pltpu.with_memory_space_constraint(a, pltpu.HBM) for a in (spectrum, source_shifts.T, source_weights[None], pupil_mask)))


def image_kernel(
    shifts, weights, spec_ref, masks, row_ref, col_ref, out_ref, flips, acc, folded, inner, live_row, live_col, live_weight
):
    src_count, _, slots = weights.shape
    source_count = src_count * slots
    mask_width = spec_ref.shape[2]
    part = spec_ref.shape[3]
    half = masks.shape[1]
    tiles = mask_width // LANES
    block = 256

    turn = reversal(block)
    for plane in range(2):
        for i in range(mask_width // block):
            for j in range(mask_width // block):
                ri, rj = mask_width // block - 1 - i, mask_width // block - 1 - j
                rows = slice(block * i, block * (i + 1))
                cells = [spec_ref[k, plane, rows] for k in range(block * j // part, -(-block * (j + 1) // part))]
                cell = cells[0] if len(cells) == 1 else jnp.concatenate(cells, axis=1)
                col_flip = dot(cell, turn)
                row_flip = dot(turn, cell)
                both = dot(turn, col_flip.astype(jnp.bfloat16))
                for version, value, vi, vj in (
                    (0, cell.astype(jnp.float32), i, j),
                    (1, row_flip, ri, j),
                    (2, col_flip, i, rj),
                    (3, both, ri, rj),
                ):
                    for t in range(block // LANES):
                        slot = (version * 2 + plane) * tiles + vj * (block // LANES) + t
                        flips[slot, block * vi : block * (vi + 1), :] = value[:, LANES * t : LANES * (t + 1)]

    def pick(i, count):
        group, slot = i // slots, lax.rem(i, slots)
        weight = weights[group, 0, slot]
        live_row[count] = shifts[group, 0, slot]
        live_col[count] = shifts[group, 1, slot]
        live_weight[count + 1] = weight
        return count + (weight > 0).astype(jnp.int32)

    live_weight[0] = 0
    count = lax.fori_loop(0, source_count, pick, jnp.int32(0))
    for g in range(GROUP + 1):
        live_row[count + g] = 0
        live_col[count + g] = 0
        live_weight[count + 1 + g] = 0

    acc[...] = jnp.zeros_like(acc)
    lane = lax.broadcasted_iota(jnp.int32, (half, LANES), 1)

    def fold(a, b, slot):
        row_offsets = (a + half, mask_width - half - a)
        col_offsets = (b + half, mask_width - half - b)
        parts = []
        for plane in range(2):
            quads = []
            for col_side in range(2):
                off = col_offsets[col_side]
                tile, rest = off // LANES, off % LANES
                after = jnp.minimum(tile + 1, tiles - 1)
                back = (LANES - rest) % LANES
                for row_side in range(2):
                    version = 2 * col_side + row_side
                    base = (version * 2 + plane) * tiles
                    rows = pl.ds(row_offsets[row_side], half)
                    left = flips[base + tile, rows, :]
                    right = flips[base + after, rows, :]
                    merged = jnp.where(lane >= rest, left, right)
                    quads.append(pltpu.roll(merged, back, 1) * masks[version])
            s1, d1 = quads[0] + quads[1], quads[0] - quads[1]
            s2, d2 = quads[2] + quads[3], quads[2] - quads[3]
            parts.append((s1, d1, s2, d2))
        (s1, d1, s2, d2), (t1, e1, t2, e2) = parts
        rows = (
            (s1 + s2, t2 - t1),
            (-(e1 + e2), d2 - d1),
            (t1 + t2, s1 - s2),
            (d1 + d2, e2 - e1),
        )
        for n, row in enumerate(rows):
            for m, value in enumerate(row):
                slot[half * n : half * (n + 1), half * m : half * (m + 1)] = value.astype(jnp.bfloat16)

    def step(n, parity):
        fold(live_row[n + 1], live_col[n + 1], folded[1 - parity])
        inner[parity][...] = dot(folded[parity][...], col_ref[...]).astype(jnp.bfloat16)
        weight = live_weight[n].astype(jnp.float32)
        real = dot(row_ref[...], inner[1 - parity][: 2 * half])
        imag = dot(row_ref[...], inner[1 - parity][2 * half :])
        acc[...] += weight * (real * real + imag * imag)

    inner[1][...] = jnp.zeros_like(inner[1])
    fold(live_row[0], live_col[0], folded[0])

    def turn_body(turn_index, carry):
        for g in range(GROUP):
            step(turn_index * GROUP + g, g % 2)
        return carry

    lax.fori_loop(0, (count + GROUP) // GROUP, turn_body, 0)
    out_ref[...] = 1.0 - jnp.exp(-(acc[...] / (2.0 * source_count)))


def image(spectrum, shifts, weights, row_table, col_table, masks):
    source_count = weights.shape[0] * weights.shape[2]
    mask_width = spectrum.shape[2]
    tile = (row_table.shape[0], col_table.shape[1])
    smem = pl.BlockSpec(memory_space=pltpu.SMEM)
    vmem = pl.BlockSpec(memory_space=pltpu.VMEM)
    return pl.pallas_call(
        image_kernel,
        out_shape=jax.ShapeDtypeStruct(tile, jnp.float32),
        in_specs=[smem, smem, vmem, vmem, vmem, vmem],
        out_specs=vmem,
        scratch_shapes=[
            pltpu.VMEM((8 * mask_width // LANES, mask_width, LANES), jnp.float32),
            pltpu.VMEM(tile, jnp.float32),
            [pltpu.VMEM((2 * row_table.shape[1], row_table.shape[1]), jnp.bfloat16)] * 2,
            [pltpu.VMEM((2 * row_table.shape[1], tile[1]), jnp.bfloat16)] * 2,
        ]
        + [pltpu.SMEM((source_count + GROUP + 2,), jnp.int32)] * 3,
        compiler_params=pltpu.CompilerParams(vmem_limit_bytes=28 << 20),
        name="image",
    )(shifts, weights, spectrum, masks, row_table, col_table)


def exchange_kernel(sizes, acid_ref, edges, beside, corners, strips, send_sem, recv_sem):
    tx_count, ty_count, src_count = sizes
    rows, cols = acid_ref.shape
    row_block = lax.axis_index("tx") * src_count + lax.axis_index("src")
    col_block = lax.axis_index("ty")
    row_blocks = tx_count * src_count

    def device(dr, dc):
        other = lax.rem(row_block + row_blocks + dr, row_blocks)
        return {
            "tx": other // src_count,
            "src": lax.rem(other, src_count),
            "ty": lax.rem(col_block + ty_count + dc, ty_count),
        }

    around = [(dr, dc) for dr in (-1, 0, 1) for dc in (-1, 0, 1) if (dr, dc) != (0, 0)]
    barrier = pltpu.get_barrier_semaphore()
    for dr, dc in around:
        pl.semaphore_signal(barrier, inc=1, device_id=device(dr, dc), device_id_type=MESH)
    strips[0] = acid_ref[:, :LANES].T[:8]
    strips[1] = acid_ref[:, cols - LANES :].T[LANES - 8 :]
    pl.semaphore_wait(barrier, len(around))

    copies = []
    for n, (dr, dc) in enumerate(around):
        if dc == 0:
            src = acid_ref.at[:8] if dr < 0 else acid_ref.at[rows - 8 :]
            dst = edges.at[0 if dr > 0 else 1]
        elif dr == 0:
            src = strips.at[0 if dc < 0 else 1]
            dst = beside.at[0 if dc > 0 else 1]
        else:
            row_part = slice(0, 8) if dr < 0 else slice(rows - 8, rows)
            col_part = slice(0, LANES) if dc < 0 else slice(cols - LANES, cols)
            src = acid_ref.at[row_part, col_part]
            dst = corners.at[(0 if dr > 0 else 2) + (0 if dc > 0 else 1)]
        copy = pltpu.make_async_remote_copy(
            src_ref=src,
            dst_ref=dst,
            send_sem=send_sem.at[n],
            recv_sem=recv_sem.at[n],
            device_id=device(dr, dc),
            device_id_type=MESH,
        )
        copy.start()
        copies.append(copy)
    for copy in copies:
        copy.wait()


def diffuse_kernel(sizes, acid_ref, edges, beside, corners, out_ref):
    tx_count, ty_count, src_count = sizes
    rows, cols = acid_ref.shape
    none = jnp.zeros((LANES - 8, rows), jnp.float32)
    left = jnp.concatenate([none, beside[0]], axis=0).T
    right = jnp.concatenate([beside[1], none], axis=0).T
    level = jnp.concatenate(
        [
            jnp.concatenate([corners[0], edges[0], corners[1]], axis=1),
            jnp.concatenate([left, acid_ref[...], right], axis=1),
            jnp.concatenate([corners[2], edges[1], corners[3]], axis=1),
        ],
        axis=0,
    )
    row_block = lax.axis_index("tx") * src_count + lax.axis_index("src")
    col_block = lax.axis_index("ty")
    row_blocks = tx_count * src_count
    x = row_block * rows - 8 + lax.broadcasted_iota(jnp.int32, level.shape, 0)
    y = col_block * cols - LANES + lax.broadcasted_iota(jnp.int32, level.shape, 1)
    inside = (x >= 0) & (x < row_blocks * rows) & (y >= 0) & (y < ty_count * cols)
    tall, wide = level.shape
    for repeat in range(2):
        level = jnp.where(inside, level, 0.0)
        near = (
            pltpu.roll(level, 1, 0)
            + pltpu.roll(level, tall - 1, 0)
            + pltpu.roll(level, 1, 1)
            + pltpu.roll(level, wide - 1, 1)
        )
        level = level + diffusion_rate * (near - 4.0 * level)
    out_ref[...] = level[8 : 8 + rows, LANES : LANES + cols]


def diffuse(acid, sizes):
    rows, cols = acid.shape
    vmem = pl.BlockSpec(memory_space=pltpu.VMEM)
    around = pl.pallas_call(
        functools.partial(exchange_kernel, sizes),
        out_shape=(
            jax.ShapeDtypeStruct((2, 8, cols), jnp.float32),
            jax.ShapeDtypeStruct((2, 8, rows), jnp.float32),
            jax.ShapeDtypeStruct((4, 8, LANES), jnp.float32),
        ),
        in_specs=[vmem],
        out_specs=(vmem,) * 3,
        scratch_shapes=[
            pltpu.VMEM((2, 8, rows), jnp.float32),
            pltpu.SemaphoreType.DMA((8,)),
            pltpu.SemaphoreType.DMA((8,)),
        ],
        compiler_params=pltpu.CompilerParams(collective_id=1, has_side_effects=True, vmem_limit_bytes=4 << 20),
        name="exchange",
    )(acid)
    return pl.pallas_call(
        functools.partial(diffuse_kernel, sizes),
        out_shape=jax.ShapeDtypeStruct((rows, cols), jnp.float32),
        in_specs=[vmem] * 4,
        out_specs=vmem,
        compiler_params=pltpu.CompilerParams(vmem_limit_bytes=12 << 20),
        name="diffuse",
    )(acid, *around)


def body(sizes, spectrum, pupil_mask, source_shifts, source_weights):
    pieces, shifts, weights, row_table, col_table, masks = gather(
        spectrum, source_shifts, source_weights, pupil_mask, sizes
    )
    src_count, _, tx_count, ty_count, block_rows, block_cols = pieces.shape
    columns = pieces.reshape(src_count, 2, tx_count * ty_count * block_rows, block_cols)
    acid = image(columns, shifts, weights, row_table, col_table, masks)
    return diffuse(acid, sizes)


def solution(mesh):
    sizes = (mesh.shape["tx"], mesh.shape["ty"], mesh.shape["src"])
    placed = (P(None, ("tx", "ty"), "src"), P(), P("src", None), P("src"))
    return jax.shard_map(
        functools.partial(body, sizes),
        mesh=mesh,
        in_specs=placed,
        out_specs=P(("tx", "src"), "ty"),
        check_vma=False,
    )
```
